256 devices in a mesh: row: 8 (over y, core), col: 32 (over x, z).
Axes of the slice: x: 4, y: 4, z: 8, core: 2. Of those that a mesh axis runs over, the one named last changes fastest.
Arguments:
- phases: int32 [8, 32, 8, 24, 576], P('row', 'col'), may hold values from 0 to 2
- grain: float32 [8, 32, 8, 24, 576], P('row', 'col'), may hold values from 0.5 to 2
- phase_cond: float32 [3], replicated, may hold values from 0.3 to 3
- micro_counts: int32 [8, 32, 8], P('row', 'col'), may hold values from 6 to 12, as said below
- current: float32 [8, 32, 8], P('row', 'col'), may hold values from -5 to 5
- load: float32 [8, 32, 8], P('row', 'col'), may hold values from -16 to 16
Outputs:
- states: float32 [8, 32, 8, 3, 24, 576], P('row', 'col')
- tangent: float32 [8, 32, 8, 3, 3], P('row', 'col')
- increment: float32 [8, 32, 8], P('row', 'col')
- residual: float32 [8, 32, 8], P('row', 'col')
The draws below stay inside these ranges and needn't reach their ends.
Inputs may be any that keep to these rules, and one draw needn't show every extreme that they name: `micro_counts`: every draw has an element with 12 inner iterations and one with 6.
All inputs are finite; a program needn't handle non-finite values.
Results may differ from the reference program's by a relative error of at most 0.0003.
Values sent between devices are 32-bit elements; how exact they have to be, the bound alone decides.
No kernel may reach another device: no remote copies, remote signals or barrier semaphores. Data moves between devices by JAX's collectives and lax.ppermute only.
A program may use at most 64 MiB of HBM per device.

```python
import math
import jax
import jax.numpy as jnp
from jax import lax

VOX = 24
YZ = 576
PHASES = 3
EZ = 8
MICRO_MAX = 12
MICRO_MIN = 6
MACRO_ITERS = 8
NEX = 8
NEY = 32


def draw_micro_counts(key, part):
    first_key, second_key = jax.random.split(jax.random.fold_in(key, 11))
    base = jax.random.randint(first_key, (NEX, NEY, 1), MICRO_MIN, MICRO_MAX + 1)
    jitter = jax.random.randint(second_key, (NEX, NEY, EZ), -1, 2)
    counts = jnp.clip(base + jitter, MICRO_MIN, MICRO_MAX)
    counts = counts.at[0, 0, 0].set(MICRO_MAX).at[0, 0, 1].set(MICRO_MIN)
    return counts.astype(jnp.int32)


def draw_load(key, part):
    along_x = jnp.arange(NEX, dtype=jnp.float32)[:, None, None] / (NEX - 1)
    along_y = jnp.arange(NEY, dtype=jnp.float32)[None, :, None] / (NEY - 1)
    scale = (1.0 + along_x) * (1.0 + along_y)
    sub_key = jax.random.fold_in(key, 23)
    values = jnp.clip(jax.random.normal(sub_key, (NEX, NEY, EZ), jnp.float32), -4.0, 4.0)
    return (scale * values).astype(jnp.float32)


def plant(entries, own_key, least, high):
    spot = [jax.random.randint(jax.random.fold_in(own_key, axis), (), 0, length) for axis, length in enumerate(entries.shape)]
    longest = entries.shape.index(max(entries.shape))
    next_to = spot[:longest] + [(spot[longest] + 1) % entries.shape[longest]] + spot[longest + 1:]
    return entries.at[tuple(spot)].set(least).at[tuple(next_to)].set(high)


def block_levels(stream_key, extent, shards, least, top_value):
    def one(position, shards_of):
        heights = jax.random.uniform(jax.random.fold_in(jax.random.fold_in(stream_key, 6), position), (shards_of,), jnp.float32, least / len(shards), top_value / len(shards))
        return jnp.repeat(jnp.exp(heights), extent[position] // shards_of).reshape((-1,) + (1,) * (len(extent) - position - 1))

    loudness = one(*shards[0])
    for cut in shards[1:]:
        loudness = loudness * one(*cut)
    return loudness


def noise(rng, shape, deviation, most, cuts=(), kind=jnp.bfloat16):
    gain = block_levels(rng, shape, cuts, -0.22, 0.18) if cuts else 1.0
    entries = jax.random.normal(rng, shape, jnp.float32) * deviation * gain
    return jnp.minimum(jnp.maximum(entries, -most), most).astype(kind)


def setup_inputs(seed: int = 0) -> dict:
    seeds = jax.random.split(jax.random.key(seed), 7)
    phases = plant(jax.random.randint(seeds[0], (NEX, NEY, EZ, VOX, YZ), 0, PHASES), jax.random.fold_in(seeds[0], 1), 0, PHASES - 1).astype(jnp.int32)
    grain = jnp.clip(jnp.exp(math.log(2.0) - 1.3862944 * jax.random.uniform(seeds[1], (NEX, NEY, EZ, VOX, YZ), jnp.float32) ** block_levels(seeds[1], (NEX, NEY, EZ, VOX, YZ), ((0, 8), (1, 32)), -0.2, 0.2)), 0.5, 2.0)
    phase_cond = jnp.clip(jnp.exp(jax.random.uniform(seeds[2], (PHASES,), jnp.float32, math.log(0.3), math.log(3.0))), 0.3, 3.0)
    micro_counts = draw_micro_counts(jax.random.fold_in(seeds[6], 71), 0)
    current = noise(seeds[4], (NEX, NEY, EZ), 1.0, 5.0, ((0, 8), (1, 32)), jnp.float32)
    load = draw_load(jax.random.fold_in(seeds[6], 71), 0)
    return {"phases": phases, "grain": grain, "phase_cond": phase_cond, "micro_counts": micro_counts, "current": current, "load": load}


def forward(field, axis_id):
    z_index = jnp.arange(YZ) % VOX
    if axis_id == 0:
        return jnp.roll(field, -1, axis=-2)
    if axis_id == 1:
        return jnp.roll(field, -VOX, axis=-1)
    return jnp.where(z_index == VOX - 1, jnp.roll(field, VOX - 1, axis=-1), jnp.roll(field, -1, axis=-1))


def behind(field, axis_id):
    z_index = jnp.arange(YZ) % VOX
    if axis_id == 0:
        return jnp.roll(field, 1, axis=-2)
    if axis_id == 1:
        return jnp.roll(field, VOX, axis=-1)
    return jnp.where(z_index == 0, jnp.roll(field, 1 - VOX, axis=-1), jnp.roll(field, 1, axis=-1))


def solve_rve(conduct, count):
    faces = [(conduct + forward(conduct, axis_id)) * 0.5 for axis_id in range(3)]
    back_faces = [behind(faces[axis_id], axis_id) for axis_id in range(3)]
    rhs = jnp.stack([faces[axis_id] - back_faces[axis_id] for axis_id in range(3)])

    def operate(field):
        total = jnp.zeros_like(field)
        for axis_id in range(3):
            total = total + faces[axis_id] * (field - forward(field, axis_id))
            total = total + back_faces[axis_id] * (field - behind(field, axis_id))
        return total

    def sweep(index, carry):
        fluct, remain, direction, norm_now = carry
        image = operate(direction)
        step_size = norm_now / jnp.sum(direction * image, axis=(1, 2))
        fluct = fluct + step_size[:, None, None] * direction
        remain = remain - step_size[:, None, None] * image
        norm_next = jnp.sum(remain * remain, axis=(1, 2))
        direction = remain + (norm_next / norm_now)[:, None, None] * direction
        return fluct, remain, direction, norm_next

    start = (jnp.zeros_like(rhs), rhs, rhs, jnp.sum(rhs * rhs, axis=(1, 2)))
    fluct = lax.fori_loop(0, count, sweep, start)[0]
    identity = jnp.eye(3, dtype=conduct.dtype)
    rows_out = []
    for axis_id in range(3):
        flux = faces[axis_id][None] * (identity[axis_id][:, None, None] + forward(fluct, axis_id) - fluct)
        rows_out.append(jnp.mean(flux, axis=(1, 2)))
    return fluct, jnp.stack(rows_out)


def neighbour(padded, axis_id, offset):
    lead = padded.ndim - 3
    index = [slice(None)] * lead + [slice(1, -1)] * 3
    length = padded.shape[lead + axis_id]
    index[lead + axis_id] = slice(1 + offset, length - 1 + offset)
    return padded[tuple(index)]


def coarse_apply(k_padded, v_padded):
    centre = neighbour(v_padded, 0, 0)
    total = jnp.zeros_like(centre)
    for axis_id in range(3):
        k_centre = neighbour(k_padded[axis_id], 0, 0)
        for offset in (1, -1):
            cond_face = 0.5 * (k_centre + neighbour(k_padded[axis_id], axis_id, offset))
            total = total + cond_face * (centre - neighbour(v_padded, axis_id, offset))
    return total


def reference(phases, grain, phase_cond, micro_counts, current, load):
    conduct = jnp.zeros(grain.shape, grain.dtype)
    for phase_id in range(PHASES):
        conduct = conduct + jnp.where(phases == phase_id, phase_cond[phase_id], 0.0)
    conduct = conduct * grain
    flat = conduct.reshape(-1, VOX, YZ)
    counts = micro_counts.reshape(-1).astype(jnp.int32)
    fluct, tangent = lax.map(lambda pair: solve_rve(pair[0], pair[1]), (flat, counts))
    states = fluct.reshape(NEX, NEY, EZ, 3, VOX, YZ)
    tangent = tangent.reshape(NEX, NEY, EZ, 3, 3)
    diag = jnp.stack([tangent[..., axis_id, axis_id] for axis_id in range(3)])
    k_padded = jnp.pad(diag, ((0, 0), (1, 1), (1, 1), (1, 1)))
    residual = load - coarse_apply(k_padded, jnp.pad(current, 1))
    increment = jnp.zeros_like(residual)
    direction = residual
    norm_now = jnp.sum(residual * residual)
    for iteration in range(MACRO_ITERS):
        image = coarse_apply(k_padded, jnp.pad(direction, 1))
        step_size = norm_now / jnp.sum(direction * image)
        increment = increment + step_size * direction
        residual = residual - step_size * image
        norm_next = jnp.sum(residual * residual)
        direction = residual + (norm_next / norm_now) * direction
        norm_now = norm_next
    return states, tangent, increment, residual
```

```python
import functools

import jax
import jax.numpy as jnp
import numpy as np
from jax import lax
from jax.experimental import pallas as pl
from jax.experimental.pallas import tpu as pltpu
from jax.sharding import Mesh
from jax.sharding import PartitionSpec as P

VOX = 24
YZ = 576
DEPTH = 8
CELLS = 27
MACRO_ITERS = 8
ROW_COL = ("row_0", "row_1", "col_0", "col_1")
ROW = ("row_0", "row_1")
COL = ("col_0", "col_1")
NEX = 8
NEY = 32
DEVICES = NEX * NEY


def block_order():
    yi, zi, yb, zb = np.meshgrid(np.arange(3), np.arange(3), np.arange(8), np.arange(8), indexing="ij")
    return ((3 * yb + yi) * VOX + 3 * zb + zi).reshape(-1)


def block_matrices():
    order = block_order()
    into = np.zeros((YZ, YZ), np.float32)
    into[order, np.arange(YZ)] = 1.0
    back = np.zeros((640, YZ), np.float32)
    back[np.arange(YZ), order] = 1.0
    return into, back


def at(xi, yi, zi):
    return xi * 9 + yi * 3 + zi


def micro_kernel(
    cond_ref,
    count_ref,
    current_ref,
    load_ref,
    phase_ref,
    grain_ref,
    into_ref,
    back_ref,
    states_ref,
    tangent_ref,
    packed_ref,
    native,
    blocked,
    face,
    edge,
    rhs0,
    res,
    way,
    flu,
    img,
    halo,
    alphas,
    betas,
    norms,
):
    f32 = jnp.float32
    lane = lax.broadcasted_iota(jnp.int32, (8, 128), 1)
    sub = lax.broadcasted_iota(jnp.int32, (8, 128), 0)
    low = lane < 64
    zb = lane & 7
    yb = (lane >> 3) & 7
    z_last, z_first = zb == 7, zb == 0
    y_last, y_first = yb == 7, yb == 0

    def roll(v, shift, axis):
        return pltpu.roll(v, shift, axis)

    ahead = (
        lambda v: roll(v, 7, 0),
        lambda v: jnp.where(y_last, roll(v, 56, 1), roll(v, 120, 1)),
        lambda v: jnp.where(z_last, roll(v, 7, 1), roll(v, 127, 1)),
    )
    before = (
        lambda v: roll(v, 1, 0),
        lambda v: jnp.where(y_first, roll(v, 72, 1), roll(v, 8, 1)),
        lambda v: jnp.where(z_first, roll(v, 121, 1), roll(v, 1, 1)),
    )

    def coords(cell):
        return cell // 9, (cell // 3) % 3, cell % 3

    def side(cell, axis):
        xi, yi, zi = coords(cell)
        return (yi * 3 + zi, xi * 3 + zi, xi * 3 + yi)[axis]

    def moved(cell, axis, step):
        where_at = list(coords(cell))
        where_at[axis] += step
        return at(*where_at)

    def both_halves(acc):
        acc = acc + roll(acc, 4, 0)
        acc = acc + roll(acc, 2, 0)
        acc = acc + roll(acc, 1, 0)
        first = jnp.sum(jnp.where(low, acc, 0.0), axis=1, keepdims=True)
        second = jnp.sum(jnp.where(low, 0.0, acc), axis=1, keepdims=True)
        return first, second

    def total(acc):
        first, second = both_halves(acc)
        return jnp.where(low, first, second)

    phase = phase_ref[...]
    conduct = jnp.where(phase == 0, cond_ref[0], jnp.where(phase == 1, cond_ref[1], cond_ref[2])) * grain_ref[...]
    part_a = conduct.astype(jnp.bfloat16)
    rest = conduct - part_a.astype(f32)
    part_b = rest.astype(jnp.bfloat16)
    part_c = (rest - part_b.astype(f32)).astype(jnp.bfloat16)
    into = into_ref[...]
    ordered = (
        jnp.dot(part_a, into, preferred_element_type=f32)
        + jnp.dot(part_b, into, preferred_element_type=f32)
        + jnp.dot(part_c, into, preferred_element_type=f32)
    )
    for t in range(4):
        native[t] = ordered[:, t * 128 : (t + 1) * 128]
    native[4, :, 0:64] = ordered[:, 512:576]

    for pair in range(4):
        cells = []
        for xi in range(3):
            for g in range(9):
                first = native[g // 2, pl.ds(2 * pair * VOX + xi, 8, stride=3), :]
                second = native[g // 2, pl.ds((2 * pair + 1) * VOX + xi, 8, stride=3), :]
                if g % 2 == 0:
                    cells.append(jnp.where(low, first, roll(second, 64, 1)))
                else:
                    cells.append(jnp.where(low, roll(first, 64, 1), second))
        for axis in range(3):
            faces = []
            for cell in range(CELLS):
                if coords(cell)[axis] < 2:
                    nxt = cells[moved(cell, axis, 1)]
                else:
                    nxt = ahead[axis](cells[moved(cell, axis, -2)])
                faces.append((cells[cell] + nxt) * 0.5)
                face[pair, axis, cell] = faces[cell]
            acc = None
            for cell in range(CELLS):
                if coords(cell)[axis] > 0:
                    back = faces[moved(cell, axis, -1)]
                else:
                    back = before[axis](faces[moved(cell, axis, 2)])
                    edge[pair, axis, side(cell, axis)] = back
                value = faces[cell] - back
                rhs0[pair, axis, cell] = value
                res[pair, axis, cell] = value
                way[pair, axis, cell] = value
                flu[pair, axis, cell] = jnp.zeros((8, 128), f32)
                acc = value * value if acc is None else acc + value * value
            norms[pair, axis] = total(acc)
            alphas[pair, axis] = jnp.zeros((8, 128), f32)
            betas[pair, axis] = jnp.zeros((8, 128), f32)

    def halves_of(pair):
        return jnp.where(low, count_ref[2 * pair], count_ref[2 * pair + 1])

    chains = [(pair, c) for pair in range(4) for c in range(3)]

    def sweep(k, carry):
        for pair, c in chains:
            alpha, beta = alphas[pair, c], betas[pair, c]
            for cell in range(CELLS):
                old = way[pair, c, cell]
                flu[pair, c, cell] = flu[pair, c, cell] + alpha * old
                new = res[pair, c, cell] + beta * old
                way[pair, c, cell] = new
                for axis in range(3):
                    if coords(cell)[axis] == 0:
                        halo[pair, c, 2 * axis, side(cell, axis)] = ahead[axis](new)
                    if coords(cell)[axis] == 2:
                        halo[pair, c, 2 * axis + 1, side(cell, axis)] = before[axis](new)
        for pair, c in chains:
            flow = {}
            acc = None
            for cell in range(CELLS):
                here = way[pair, c, cell]
                out = None
                for axis in range(3):
                    spot = coords(cell)[axis]
                    if spot < 2:
                        nxt = way[pair, c, moved(cell, axis, 1)]
                    else:
                        nxt = halo[pair, c, 2 * axis, side(cell, axis)]
                    flux = face[pair, axis, cell] * (here - nxt)
                    if spot > 0:
                        back = flow.pop((axis, moved(cell, axis, -1)))
                    else:
                        back = edge[pair, axis, side(cell, axis)] * (halo[pair, c, 2 * axis + 1, side(cell, axis)] - here)
                    if spot < 2:
                        flow[axis, cell] = flux
                    out = flux - back if out is None else out + (flux - back)
                img[pair, c, cell] = out
                acc = here * out if acc is None else acc + here * out
            alpha = norms[pair, c] / total(acc)
            alphas[pair, c] = jnp.where(halves_of(pair) > k, alpha, 0.0)
        for pair, c in chains:
            alpha = alphas[pair, c]
            acc = None
            for cell in range(CELLS):
                value = res[pair, c, cell] - alpha * img[pair, c, cell]
                res[pair, c, cell] = value
                acc = value * value if acc is None else acc + value * value
            new = total(acc)
            betas[pair, c] = jnp.where(halves_of(pair) > k, new / norms[pair, c], 0.0)
            norms[pair, c] = new
        return carry

    most = count_ref[0]
    for e in range(1, DEPTH):
        most = jnp.maximum(most, count_ref[e])
    lax.fori_loop(0, most, sweep, 0)

    share = 1.0 / (VOX * YZ)
    packed = jnp.zeros((8, 128), f32)
    tangents = [jnp.zeros((8, 128), f32) for _ in range(DEPTH)]
    for pair in range(4):
        for c in range(3):
            alpha = alphas[pair, c]
            accs = [None] * 3
            for xi in range(3):
                row = []
                for g in range(9):
                    cell = xi * 9 + g
                    value = flu[pair, c, cell] + alpha * way[pair, c, cell]
                    row.append(value)
                    for d in range(3):
                        term = value * rhs0[pair, d, cell]
                        if d == c:
                            term = term - face[pair, d, cell]
                        accs[d] = term if accs[d] is None else accs[d] + term
                start = (2 * pair * 3 + c) * VOX + xi
                for t in range(5):
                    if t < 4:
                        one = jnp.where(low, row[2 * t], roll(row[2 * t + 1], 64, 1))
                        two = jnp.where(low, roll(row[2 * t], 64, 1), row[2 * t + 1])
                    else:
                        one = jnp.where(low, row[8], 0.0)
                        two = jnp.where(low, roll(row[8], 64, 1), 0.0)
                    blocked[t, pl.ds(start, 8, stride=3), :] = one
                    blocked[t, pl.ds(start + 3 * VOX, 8, stride=3), :] = two
            for d in range(3):
                for half, value in enumerate(both_halves(accs[d])):
                    e = 2 * pair + half
                    value = value * (-share)
                    tangents[e] = jnp.where((sub == d) & (lane == c), value, tangents[e])
                    if d == c:
                        packed = jnp.where(lane == d * DEPTH + e, value, packed)
    for e in range(DEPTH):
        tangent_ref[e] = tangents[e][0:3, 0:3]
        packed = jnp.where(lane == 3 * DEPTH + e, current_ref[e], packed)
        packed = jnp.where(lane == 4 * DEPTH + e, load_ref[e], packed)
    for block in range(DEVICES // 8):
        packed_ref[block * 8 : block * 8 + 8, :] = packed

    back = back_ref[...]
    for m in range(3):
        rows = pl.ds(m * 192, 192)
        lhs = jnp.concatenate([blocked[t, rows, :] for t in range(5)], axis=1)
        upper = lhs.astype(jnp.bfloat16)
        lower = (lhs - upper.astype(f32)).astype(jnp.bfloat16)
        states_ref[rows, :] = jnp.dot(upper, back, preferred_element_type=f32) + jnp.dot(
            lower, back, preferred_element_type=f32
        )


def solve_cells(phases, grain, phase_cond, counts, current, load):
    into, back = block_matrices()
    f32 = jnp.float32
    smem = pl.BlockSpec(memory_space=pltpu.SMEM)
    vmem = pl.BlockSpec(memory_space=pltpu.VMEM)
    field = pltpu.VMEM((4, 3, CELLS, 8, 128), f32)
    return pl.pallas_call(
        micro_kernel,
        out_shape=(
            jax.ShapeDtypeStruct((DEPTH * 3 * VOX, YZ), f32),
            jax.ShapeDtypeStruct((DEPTH, 3, 3), f32),
            jax.ShapeDtypeStruct((DEVICES, 128), f32),
        ),
        in_specs=[smem] * 4 + [vmem] * 4,
        out_specs=(vmem, vmem, vmem),
        scratch_shapes=[
            pltpu.VMEM((5, DEPTH * VOX, 128), f32),
            pltpu.VMEM((5, DEPTH * 3 * VOX, 128), f32),
            field,
            pltpu.VMEM((4, 3, 9, 8, 128), f32),
            field,
            field,
            field,
            field,
            field,
            pltpu.VMEM((4, 3, 6, 9, 8, 128), f32),
            pltpu.VMEM((4, 3, 8, 128), f32),
            pltpu.VMEM((4, 3, 8, 128), f32),
            pltpu.VMEM((4, 3, 8, 128), f32),
        ],
        compiler_params=pltpu.CompilerParams(vmem_limit_bytes=40 * 1024 * 1024),
        name="cells",
    )(
        phase_cond,
        counts,
        current,
        load,
        phases,
        grain,
        jnp.asarray(into, jnp.bfloat16),
        jnp.asarray(back, jnp.bfloat16),
    )


def coarse_kernel(place_ref, packed_ref, increment_ref, residual_ref):
    f32 = jnp.float32
    nodes = packed_ref[...].T
    shape = (DEPTH, DEVICES)
    lane = lax.broadcasted_iota(jnp.int32, shape, 1)
    sub = lax.broadcasted_iota(jnp.int32, shape, 0)
    col, row = lane & (NEY - 1), lane >> 5
    has_next = (row < NEX - 1, col < NEY - 1, sub < DEPTH - 1)
    has_back = (row > 0, col > 0, sub > 0)

    def following(v, axis):
        if axis == 2:
            return pltpu.roll(v, DEPTH - 1, 0)
        return pltpu.roll(v, DEVICES - (NEY if axis == 0 else 1), 1)

    def preceding(v, axis):
        if axis == 2:
            return pltpu.roll(v, 1, 0)
        return pltpu.roll(v, NEY if axis == 0 else 1, 1)

    def total(v):
        v = v[:, :128] + v[:, 128:]
        v = v + pltpu.roll(v, 4, 0)
        v = v + pltpu.roll(v, 2, 0)
        v = v + pltpu.roll(v, 1, 0)
        return jnp.sum(v, axis=1, keepdims=True)

    own = None
    links = []
    for axis in range(3):
        k = nodes[axis * DEPTH : (axis + 1) * DEPTH]
        for shift, inside in ((following, has_next[axis]), (preceding, has_back[axis])):
            other = jnp.where(inside, shift(k, axis), 0.0)
            mean = 0.5 * (k + other)
            own = mean if own is None else own + mean
            links.append((shift, axis, jnp.where(inside, mean, 0.0)))

    def apply(v):
        out = own * v
        for shift, axis, weight in links:
            out = out - weight * shift(v, axis)
        return out

    current = nodes[3 * DEPTH : 4 * DEPTH]
    residual = nodes[4 * DEPTH : 5 * DEPTH] - apply(current)
    increment = jnp.zeros(shape, f32)
    direction = residual
    norm_now = total(residual * residual)
    for _ in range(MACRO_ITERS):
        image = apply(direction)
        step = norm_now / total(direction * image)
        increment = increment + step * direction
        residual = residual - step * image
        norm_next = total(residual * residual)
        direction = residual + norm_next / norm_now * direction
        norm_now = norm_next

    spot = sub[:, :128] == lane[:, :128]
    for value, ref in ((increment, increment_ref), (residual, residual_ref)):
        column = jnp.sum(jnp.where(lane == place_ref[0], value, 0.0), axis=1, keepdims=True)
        line = jnp.sum(jnp.where(spot, column, 0.0), axis=0, keepdims=True)
        ref[...] = line[:, :DEPTH]


def solve_coarse(place, packed):
    smem = pl.BlockSpec(memory_space=pltpu.SMEM)
    vmem = pl.BlockSpec(memory_space=pltpu.VMEM)
    line = jax.ShapeDtypeStruct((1, DEPTH), jnp.float32)
    return pl.pallas_call(
        coarse_kernel,
        out_shape=(line, line),
        in_specs=[smem, vmem],
        out_specs=(vmem, vmem),
        name="coarse",
    )(place, packed)


def shards(phases, grain, phase_cond, micro_counts, current, load):
    states, tangent, packed = solve_cells(
        phases.reshape(DEPTH * VOX, YZ),
        grain.reshape(DEPTH * VOX, YZ),
        phase_cond,
        micro_counts.reshape(DEPTH),
        current.reshape(DEPTH),
        load.reshape(DEPTH),
    )
    whole = lax.all_to_all(packed.reshape(DEVICES, 1, 128), ROW_COL, 0, 0, tiled=True)
    place = lax.axis_index(ROW_COL).astype(jnp.int32).reshape(1)
    increment, residual = solve_coarse(place, whole.reshape(DEVICES, 128))
    return (
        states.reshape(1, 1, DEPTH, 3, VOX, YZ),
        tangent.reshape(1, 1, DEPTH, 3, 3),
        increment.reshape(1, 1, DEPTH),
        residual.reshape(1, 1, DEPTH),
    )


def solution(mesh):
    torus = Mesh(mesh.devices.reshape(4, 2, 4, 8), ("row_0", "row_1", "col_0", "col_1"))
    in_specs = (
        P(ROW, COL, None, None, None),
        P(ROW, COL, None, None, None),
        P(),
        P(ROW, COL, None),
        P(ROW, COL, None),
        P(ROW, COL, None),
    )
    out_specs = (
        P(ROW, COL, None, None, None, None),
        P(ROW, COL, None, None, None),
        P(ROW, COL, None),
        P(ROW, COL, None),
    )
    return jax.shard_map(
        shards, mesh=torus, in_specs=in_specs, out_specs=out_specs, check_vma=False
    )
```

```python
import functools

import jax
import jax.numpy as jnp
import numpy as np
from jax import lax
from jax.experimental import pallas as pl
from jax.experimental.pallas import tpu as pltpu
from jax.sharding import Mesh
from jax.sharding import PartitionSpec as P

VOX = 24
YZ = 576
DEPTH = 8
CELLS = 27
MACRO_ITERS = 8
MICRO_MAX = 12
LANE_TAKE = True
MICRO_MIN = 6
VMEM = 67_043_328
EARLY = 8
LEAD = 12
ROW_COL = ("row_0", "row_1", "col_0", "col_1")
ROW = ("row_0", "row_1")
COL = ("col_0", "col_1")
NEX = 8
NEY = 32
DEVICES = NEX * NEY


def block_order():
    yi, zi, yb, zb = np.meshgrid(np.arange(3), np.arange(3), np.arange(8), np.arange(8), indexing="ij")
    return ((3 * yb + yi) * VOX + 3 * zb + zi).reshape(-1)


def block_matrices():
    order = block_order()
    into = np.zeros((YZ, YZ), np.float32)
    into[order, np.arange(YZ)] = 1.0
    back = np.zeros((640, YZ), np.float32)
    back[np.arange(YZ), order] = 1.0
    return into, back


def at(xi, yi, zi):
    return xi * 9 + yi * 3 + zi


def helpers():
    lane = lax.broadcasted_iota(jnp.int32, (8, 128), 1)
    sub = lax.broadcasted_iota(jnp.int32, (8, 128), 0)
    low = lane < 64
    high_part, yb, zb = lane & 64, (lane >> 3) & 7, lane & 7
    y_part, z_part = lane & 56, lane & 7
    y_next = high_part | ((y_part + 8) & 56) | z_part
    y_prev = high_part | ((y_part + 56) & 56) | z_part
    z_next = high_part | y_part | ((z_part + 1) & 7)
    z_prev = high_part | y_part | ((z_part + 7) & 7)

    def taken(v, index):
        return jnp.take_along_axis(v, index, axis=1, mode="promise_in_bounds")

    if LANE_TAKE:
        ahead = (
            lambda v: pltpu.roll(v, 7, 0),
            lambda v: taken(v, y_next),
            lambda v: taken(v, z_next),
        )
        before = (
            lambda v: pltpu.roll(v, 1, 0),
            lambda v: taken(v, y_prev),
            lambda v: taken(v, z_prev),
        )
    else:
        ahead = (
            lambda v: pltpu.roll(v, 7, 0),
            lambda v: jnp.where(yb == 7, pltpu.roll(v, 56, 1), pltpu.roll(v, 120, 1)),
            lambda v: jnp.where(zb == 7, pltpu.roll(v, 7, 1), pltpu.roll(v, 127, 1)),
        )
        before = (
            lambda v: pltpu.roll(v, 1, 0),
            lambda v: jnp.where(yb == 0, pltpu.roll(v, 72, 1), pltpu.roll(v, 8, 1)),
            lambda v: jnp.where(zb == 0, pltpu.roll(v, 121, 1), pltpu.roll(v, 1, 1)),
        )

    def both_halves(acc):
        acc = acc + pltpu.roll(acc, 4, 0)
        acc = acc + pltpu.roll(acc, 2, 0)
        acc = acc + pltpu.roll(acc, 1, 0)
        first = jnp.sum(jnp.where(low, acc, 0.0), axis=1, keepdims=True)
        second = jnp.sum(jnp.where(low, 0.0, acc), axis=1, keepdims=True)
        return first, second

    def total(acc):
        first, second = both_halves(acc)
        return jnp.where(low, first, second)

    return lane, sub, low, ahead, before, both_halves, total


def coords(cell):
    return cell // 9, (cell // 3) % 3, cell % 3


def side(cell, axis):
    xi, yi, zi = coords(cell)
    return (yi * 3 + zi, xi * 3 + zi, xi * 3 + yi)[axis]


def moved(cell, axis, step):
    spot = list(coords(cell))
    spot[axis] += step
    return at(*spot)


def cells_kernel(
    cond_hbm,
    count_hbm,
    current_hbm,
    load_hbm,
    phase_hbm,
    grain_hbm,
    into_hbm,
    path_hbm,
    steps_hbm,
    rhs0_hbm,
    sums_hbm,
    packed_hbm,
    path,
    steps,
    rhs0,
    sums,
    packed_ref,
    cond_ref,
    count_ref,
    current_ref,
    load_ref,
    phase_ref,
    grain_ref,
    into_ref,
    native,
    face,
    res,
    way,
    img,
    halo,
    alphas,
    betas,
    norms,
    energy,
    partial,
    sems,
    path_sems,
):
    f32 = jnp.float32
    copies = [
        pltpu.make_async_copy(src, dst, sems.at[n])
        for n, (src, dst) in enumerate(
            (
                (phase_hbm, phase_ref),
                (grain_hbm, grain_ref),
                (into_hbm, into_ref),
                (cond_hbm, cond_ref),
                (count_hbm, count_ref),
                (current_hbm, current_ref),
                (load_hbm, load_ref),
            )
        )
    ]
    for copy in copies:
        copy.start()
    lane, sub, low, ahead, before, both_halves, total = helpers()
    zero = jnp.zeros((8, 128), f32)
    for copy in copies:
        copy.wait()

    phase = phase_ref[...]
    conduct = jnp.where(phase == 0, cond_ref[0], jnp.where(phase == 1, cond_ref[1], cond_ref[2])) * grain_ref[...]
    part_a = conduct.astype(jnp.bfloat16)
    rest = conduct - part_a.astype(f32)
    part_b = rest.astype(jnp.bfloat16)
    part_c = (rest - part_b.astype(f32)).astype(jnp.bfloat16)
    into = into_ref[...]
    ordered = (
        jnp.dot(part_a, into, preferred_element_type=f32)
        + jnp.dot(part_b, into, preferred_element_type=f32)
        + jnp.dot(part_c, into, preferred_element_type=f32)
    )
    for t in range(4):
        native[t] = ordered[:, t * 128 : (t + 1) * 128]
    native[4, :, 0:64] = ordered[:, 512:576]

    for pair in range(4):
        cells = []
        for xi in range(3):
            for g in range(9):
                first = native[g // 2, pl.ds(2 * pair * VOX + xi, 8, stride=3), :]
                second = native[g // 2, pl.ds((2 * pair + 1) * VOX + xi, 8, stride=3), :]
                if g % 2 == 0:
                    cells.append(jnp.where(low, first, pltpu.roll(second, 64, 1)))
                else:
                    cells.append(jnp.where(low, pltpu.roll(first, 64, 1), second))
        for axis in range(3):
            faces = []
            acc_face = None
            for cell in range(CELLS):
                if coords(cell)[axis] < 2:
                    nxt = cells[moved(cell, axis, 1)]
                else:
                    nxt = ahead[axis](cells[moved(cell, axis, -2)])
                value = (cells[cell] + nxt) * 0.5
                faces.append(value)
                face[pair, axis, cell] = value
                acc_face = value if acc_face is None else acc_face + value
            acc = None
            for cell in range(CELLS):
                if coords(cell)[axis] > 0:
                    back = faces[moved(cell, axis, -1)]
                else:
                    back = before[axis](faces[moved(cell, axis, 2)])
                value = faces[cell] - back
                rhs0[pair, axis, cell] = value
                res[pair, axis, cell] = value
                way[pair, axis, cell] = value
                path[0, pair, axis, cell] = value
                acc = value * value if acc is None else acc + value * value
            norms[pair, axis] = total(acc)
            sums[pair, axis] = total(acc_face)
            energy[pair, axis] = zero

    most = count_ref[0]
    for e in range(1, DEPTH):
        most = jnp.maximum(most, count_ref[e])

    rhs0_copy = pltpu.make_async_copy(rhs0, rhs0_hbm, sems.at[7])
    rhs0_copy.start()
    sums_copy = pltpu.make_async_copy(sums, sums_hbm, sems.at[8])
    sums_copy.start()

    def path_copy(k):
        return pltpu.make_async_copy(path.at[k], path_hbm.at[k], path_sems.at[k])

    path_copy(0).start()
    chains = [(pair, c) for pair in range(4) for c in range(3)]
    late = chains[EARLY:]

    def active(pair, k):
        return jnp.where(low, count_ref[2 * pair], count_ref[2 * pair + 1]) > k

    def set_step(pair, c, k, curve):
        norm = norms[pair, c]
        alpha = jnp.where(active(pair, k), norm / curve, 0.0)
        alphas[pair, c] = alpha
        steps[k, pair, c] = alpha
        energy[pair, c] = energy[pair, c] + alpha * norm

    def far_fluxes(pair, c):
        for axis in range(3):
            for cell in range(CELLS):
                if coords(cell)[axis] == 2:
                    nxt = ahead[axis](way[pair, c, moved(cell, axis, -2)])
                    halo[pair, c, 2 * axis, side(cell, axis)] = face[pair, axis, cell] * (way[pair, c, cell] - nxt)

    def near_fluxes(pair, c):
        for axis in range(3):
            for spot in range(9):
                halo[pair, c, 2 * axis + 1, spot] = before[axis](halo[pair, c, 2 * axis, spot])

    def images(k):
        for pair, c in chains:
            flow = {}
            acc = None
            for cell in range(CELLS):
                here = way[pair, c, cell]
                out = None
                for axis in range(3):
                    spot = coords(cell)[axis]
                    if spot < 2:
                        flux = face[pair, axis, cell] * (here - way[pair, c, moved(cell, axis, 1)])
                    else:
                        flux = halo[pair, c, 2 * axis, side(cell, axis)]
                    if spot > 0:
                        back = flow.pop((axis, moved(cell, axis, -1)))
                    else:
                        back = halo[pair, c, 2 * axis + 1, side(cell, axis)]
                    if spot < 2:
                        flow[axis, cell] = flux
                    out = flux - back if out is None else out + (flux - back)
                img[pair, c, cell] = out
                acc = here * out if acc is None else acc + here * out
            if (pair, c) in late:
                partial[pair, c] = acc
            else:
                set_step(pair, c, k, total(acc))

    def finish(k):
        for pair, c in late:
            set_step(pair, c, k, total(partial[pair, c]))

    for n, chain in enumerate(chains):
        far_fluxes(*chain)
        if n >= LEAD:
            near_fluxes(*chains[n - LEAD])
    for chain in chains[len(chains) - LEAD :]:
        near_fluxes(*chain)
    images(0)

    def sweep(k, carry):
        finish(k - 1)
        for pair, c in chains:
            alpha = alphas[pair, c]
            acc = None
            for cell in range(CELLS):
                value = res[pair, c, cell] - alpha * img[pair, c, cell]
                res[pair, c, cell] = value
                acc = value * value if acc is None else acc + value * value
            new = total(acc)
            betas[pair, c] = jnp.where(active(pair, k), new / norms[pair, c], 0.0)
            norms[pair, c] = new
        for n, (pair, c) in enumerate(chains):
            beta = betas[pair, c]
            for cell in range(CELLS):
                value = res[pair, c, cell] + beta * way[pair, c, cell]
                way[pair, c, cell] = value
                path[k, pair, c, cell] = value
            far_fluxes(pair, c)
            if n >= LEAD:
                near_fluxes(*chains[n - LEAD])
        path_copy(k).start()
        for chain in chains[len(chains) - LEAD :]:
            near_fluxes(*chain)
        images(k)
        return carry

    lax.fori_loop(1, most, sweep, 0)
    finish(most - 1)
    steps_copy = pltpu.make_async_copy(steps, steps_hbm, sems.at[9])
    steps_copy.start()

    share = 1.0 / (VOX * YZ)
    packed = zero
    for pair in range(4):
        for d in range(3):
            value = (sums[pair, d] - energy[pair, d]) * share
            packed = jnp.where(lane == d * DEPTH + 2 * pair, value, packed)
            packed = jnp.where(lane == d * DEPTH + 2 * pair + 1, pltpu.roll(value, 64, 1), packed)
    for e in range(DEPTH):
        packed = jnp.where(lane == 3 * DEPTH + e, current_ref[e], packed)
        packed = jnp.where(lane == 4 * DEPTH + e, load_ref[e], packed)
    for block in range(DEVICES // 8):
        packed_ref[block * 8 : block * 8 + 8, :] = packed
    packed_copy = pltpu.make_async_copy(packed_ref, packed_hbm, sems.at[10])
    packed_copy.start()

    def settle(k, carry):
        path_copy(k).wait()
        return carry

    lax.fori_loop(0, most, settle, 0)
    rhs0_copy.wait()
    sums_copy.wait()
    steps_copy.wait()
    packed_copy.wait()


def output_kernel(
    count_hbm,
    path_hbm,
    steps_hbm,
    rhs0_hbm,
    sums_hbm,
    back_hbm,
    states_hbm,
    tangent_ref,
    count_ref,
    path,
    steps,
    rhs0,
    sums,
    back_ref,
    flu,
    blocked,
    states_ref,
    sems,
    path_sems,
):
    f32 = jnp.float32
    count_copy = pltpu.make_async_copy(count_hbm, count_ref, sems.at[0])
    count_copy.start()
    steps_copy = pltpu.make_async_copy(steps_hbm, steps, sems.at[1])
    steps_copy.start()

    def path_copy(k):
        return pltpu.make_async_copy(path_hbm.at[k], path.at[k], path_sems.at[k])

    for k in range(MICRO_MIN):
        path_copy(k).start()
    copies = [
        pltpu.make_async_copy(rhs0_hbm, rhs0, sems.at[2]),
        pltpu.make_async_copy(sums_hbm, sums, sems.at[3]),
        pltpu.make_async_copy(back_hbm, back_ref, sems.at[4]),
    ]
    lane, sub, low, ahead, before, both_halves, total = helpers()
    count_copy.wait()
    most = count_ref[0]
    for e in range(1, DEPTH):
        most = jnp.maximum(most, count_ref[e])

    def begin(k, carry):
        path_copy(k).start()
        return carry

    lax.fori_loop(MICRO_MIN, most, begin, 0)
    for copy in copies:
        copy.start()
    steps_copy.wait()
    chains = [(pair, c) for pair in range(4) for c in range(3)]
    path_copy(0).wait()
    for pair, c in chains:
        alpha = steps[0, pair, c]
        for cell in range(CELLS):
            flu[pair, c, cell] = alpha * path[0, pair, c, cell]

    def add(k, carry):
        path_copy(k).wait()
        for pair, c in chains:
            alpha = steps[k, pair, c]
            for cell in range(CELLS):
                flu[pair, c, cell] = flu[pair, c, cell] + alpha * path[k, pair, c, cell]
        return carry

    lax.fori_loop(1, most, add, 0)
    for copy in copies:
        copy.wait()

    share = 1.0 / (VOX * YZ)
    row_e = lax.broadcasted_iota(jnp.int32, (16, 128), 1)
    row_d = lax.broadcasted_iota(jnp.int32, (16, 128), 0)
    tangent = jnp.zeros((16, 128), f32)
    for pair in range(4):
        for c in range(3):
            held = [flu[pair, c, cell] for cell in range(CELLS)]
            accs = [None] * 3
            for cell in range(CELLS):
                for d in range(3):
                    term = held[cell] * rhs0[pair, d, cell]
                    accs[d] = term if accs[d] is None else accs[d] + term
            for xi in range(3):
                row = held[xi * 9 : xi * 9 + 9]
                start = (2 * pair * 3 + c) * VOX + xi
                for t in range(5):
                    if t < 4:
                        one = jnp.where(low, row[2 * t], pltpu.roll(row[2 * t + 1], 64, 1))
                        two = jnp.where(low, pltpu.roll(row[2 * t], 64, 1), row[2 * t + 1])
                    else:
                        one = jnp.where(low, row[8], 0.0)
                        two = jnp.where(low, pltpu.roll(row[8], 64, 1), 0.0)
                    blocked[t, pl.ds(start, 8, stride=3), :] = one
                    blocked[t, pl.ds(start + 3 * VOX, 8, stride=3), :] = two
            for d in range(3):
                value = total(accs[d])
                value = (sums[pair, d] - value if d == c else -value) * share
                for half in range(2):
                    flat = value[0:1, 64 * half : 64 * half + 1]
                    tangent = jnp.where((row_d == 3 * d + c) & (row_e == 2 * pair + half), flat, tangent)
    for n in range(9):
        tangent_ref[n] = tangent[n : n + 1, 0:DEPTH]

    back = back_ref[...]
    states_copies = []
    for m in range(3):
        rows = pl.ds(m * 192, 192)
        lhs = jnp.concatenate([blocked[t, rows, :] for t in range(5)], axis=1)
        upper = lhs.astype(jnp.bfloat16)
        lower = (lhs - upper.astype(f32)).astype(jnp.bfloat16)
        states_ref[rows, :] = jnp.dot(upper, back, preferred_element_type=f32) + jnp.dot(
            lower, back, preferred_element_type=f32
        )
        states_copies.append(pltpu.make_async_copy(states_ref.at[rows], states_hbm.at[rows], sems.at[5 + m]))
        states_copies[m].start()
    for copy in states_copies:
        copy.wait()


def solve_cells(phases, grain, phase_cond, counts, current, load):
    into, back = block_matrices()
    f32 = jnp.float32
    hbm = pl.BlockSpec(memory_space=pltpu.HBM)
    vmem = pl.BlockSpec(memory_space=pltpu.VMEM)
    field = pltpu.VMEM((4, 3, CELLS, 8, 128), f32)
    chain = pltpu.VMEM((4, 3, 8, 128), f32)
    path, steps, rhs0, sums, packed = pl.pallas_call(
        cells_kernel,
        out_shape=(
            jax.ShapeDtypeStruct((MICRO_MAX, 4, 3, CELLS, 8, 128), f32),
            jax.ShapeDtypeStruct((MICRO_MAX, 4, 3, 8, 128), f32),
            jax.ShapeDtypeStruct((4, 3, CELLS, 8, 128), f32),
            jax.ShapeDtypeStruct((4, 3, 8, 128), f32),
            jax.ShapeDtypeStruct((DEVICES, 128), f32),
        ),
        in_specs=[hbm] * 7,
        out_specs=(hbm,) * 5,
        scratch_shapes=[
            pltpu.VMEM((MICRO_MAX, 4, 3, CELLS, 8, 128), f32),
            pltpu.VMEM((MICRO_MAX, 4, 3, 8, 128), f32),
            field,
            chain,
            pltpu.VMEM((DEVICES, 128), f32),
            pltpu.SMEM((3,), f32),
            pltpu.SMEM((DEPTH,), jnp.int32),
            pltpu.SMEM((DEPTH,), f32),
            pltpu.SMEM((DEPTH,), f32),
            pltpu.VMEM((DEPTH * VOX, YZ), jnp.int32),
            pltpu.VMEM((DEPTH * VOX, YZ), f32),
            pltpu.VMEM((YZ, YZ), jnp.bfloat16),
            pltpu.VMEM((5, DEPTH * VOX, 128), f32),
            field,
            field,
            field,
            field,
            pltpu.VMEM((4, 3, 6, 9, 8, 128), f32),
            chain,
            chain,
            chain,
            chain,
            chain,
            pltpu.SemaphoreType.DMA((11,)),
            pltpu.SemaphoreType.DMA((MICRO_MAX,)),
        ],
        compiler_params=pltpu.CompilerParams(vmem_limit_bytes=VMEM),
        name="cells",
    )(phase_cond, counts, current, load, phases, grain, jnp.asarray(into, jnp.bfloat16))

    def output():
        return pl.pallas_call(
            output_kernel,
            out_shape=(
                jax.ShapeDtypeStruct((DEPTH * 3 * VOX, YZ), f32),
                jax.ShapeDtypeStruct((9, 1, DEPTH), f32),
            ),
            in_specs=[hbm] * 6,
            out_specs=(hbm, vmem),
            scratch_shapes=[
                pltpu.SMEM((DEPTH,), jnp.int32),
                pltpu.VMEM((MICRO_MAX, 4, 3, CELLS, 8, 128), f32),
                pltpu.VMEM((MICRO_MAX, 4, 3, 8, 128), f32),
                field,
                chain,
                pltpu.VMEM((640, YZ), jnp.bfloat16),
                field,
                pltpu.VMEM((5, DEPTH * 3 * VOX, 128), f32),
                pltpu.VMEM((DEPTH * 3 * VOX, YZ), f32),
                pltpu.SemaphoreType.DMA((8,)),
                pltpu.SemaphoreType.DMA((MICRO_MAX,)),
            ],
            compiler_params=pltpu.CompilerParams(vmem_limit_bytes=VMEM),
            cost_estimate=pl.CostEstimate(flops=400_000_000, bytes_accessed=4_000_000, transcendentals=0),
            name="output",
        )(counts, path, steps, rhs0, sums, jnp.asarray(back, jnp.bfloat16))

    return packed, output


def coarse_kernel(place_ref, packed_ref, increment_ref, residual_ref):
    f32 = jnp.float32
    nodes = packed_ref[...].T
    shape = (DEPTH, DEVICES)
    lane = lax.broadcasted_iota(jnp.int32, shape, 1)
    sub = lax.broadcasted_iota(jnp.int32, shape, 0)
    col, row = lane & (NEY - 1), lane >> 5
    has_next = (row < NEX - 1, col < NEY - 1, sub < DEPTH - 1)
    has_back = (row > 0, col > 0, sub > 0)

    def following(v, axis):
        if axis == 2:
            return pltpu.roll(v, DEPTH - 1, 0)
        return pltpu.roll(v, DEVICES - (NEY if axis == 0 else 1), 1)

    def preceding(v, axis):
        if axis == 2:
            return pltpu.roll(v, 1, 0)
        return pltpu.roll(v, NEY if axis == 0 else 1, 1)

    def total(v):
        v = v[:, :128] + v[:, 128:]
        v = v + pltpu.roll(v, 4, 0)
        v = v + pltpu.roll(v, 2, 0)
        v = v + pltpu.roll(v, 1, 0)
        return jnp.sum(v, axis=1, keepdims=True)

    own = None
    links = []
    for axis in range(3):
        k = nodes[axis * DEPTH : (axis + 1) * DEPTH]
        for shift, inside in ((following, has_next[axis]), (preceding, has_back[axis])):
            other = jnp.where(inside, shift(k, axis), 0.0)
            mean = 0.5 * (k + other)
            own = mean if own is None else own + mean
            links.append((shift, axis, jnp.where(inside, mean, 0.0)))

    def apply(v):
        out = own * v
        for shift, axis, weight in links:
            out = out - weight * shift(v, axis)
        return out

    current = nodes[3 * DEPTH : 4 * DEPTH]
    residual = nodes[4 * DEPTH : 5 * DEPTH] - apply(current)
    increment = jnp.zeros(shape, f32)
    direction = residual
    norm_now = total(residual * residual)
    for _ in range(MACRO_ITERS):
        image = apply(direction)
        step = norm_now / total(direction * image)
        increment = increment + step * direction
        residual = residual - step * image
        norm_next = total(residual * residual)
        direction = residual + norm_next / norm_now * direction
        norm_now = norm_next

    spot = sub[:, :128] == lane[:, :128]
    for value, ref in ((increment, increment_ref), (residual, residual_ref)):
        column = jnp.sum(jnp.where(lane == place_ref[0], value, 0.0), axis=1, keepdims=True)
        line = jnp.sum(jnp.where(spot, column, 0.0), axis=0, keepdims=True)
        ref[...] = line[:, :DEPTH]


def solve_coarse(place, packed):
    smem = pl.BlockSpec(memory_space=pltpu.SMEM)
    vmem = pl.BlockSpec(memory_space=pltpu.VMEM)
    line = jax.ShapeDtypeStruct((1, DEPTH), jnp.float32)
    return pl.pallas_call(
        coarse_kernel,
        out_shape=(line, line),
        in_specs=[smem, vmem],
        out_specs=(vmem, vmem),
        compiler_params=pltpu.CompilerParams(vmem_limit_bytes=4 * 1024 * 1024),
        name="coarse",
    )(place, packed)


def shards(phases, grain, phase_cond, micro_counts, current, load):
    packed, output = solve_cells(
        phases.reshape(DEPTH * VOX, YZ),
        grain.reshape(DEPTH * VOX, YZ),
        phase_cond,
        micro_counts.reshape(DEPTH),
        current.reshape(DEPTH),
        load.reshape(DEPTH),
    )
    whole = lax.all_to_all(packed.reshape(DEVICES, 1, 128), ROW_COL, 0, 0, tiled=True)
    states, tangent = output()
    place = lax.axis_index(ROW_COL).astype(jnp.int32).reshape(1)
    increment, residual = solve_coarse(place, whole.reshape(DEVICES, 128))
    return (
        states.reshape(1, 1, DEPTH, 3, VOX, YZ),
        tangent.reshape(3, 3, 1, 1, DEPTH).transpose(2, 3, 4, 0, 1),
        increment.reshape(1, 1, DEPTH),
        residual.reshape(1, 1, DEPTH),
    )


def solution(mesh):
    torus = Mesh(mesh.devices.reshape(4, 2, 4, 8), ("row_0", "row_1", "col_0", "col_1"))
    in_specs = (
        P(ROW, COL, None, None, None),
        P(ROW, COL, None, None, None),
        P(),
        P(ROW, COL, None),
        P(ROW, COL, None),
        P(ROW, COL, None),
    )
    out_specs = (
        P(ROW, COL, None, None, None, None),
        P(ROW, COL, None, None, None),
        P(ROW, COL, None),
        P(ROW, COL, None),
    )
    return jax.shard_map(
        shards, mesh=torus, in_specs=in_specs, out_specs=out_specs, check_vma=False
    )
```

```python
import functools

import jax
import jax.numpy as jnp
import numpy as np
from jax import lax
from jax.experimental import pallas as pl
from jax.experimental.pallas import tpu as pltpu
from jax.sharding import Mesh
from jax.sharding import PartitionSpec as P

VOX = 24
YZ = 576
DEPTH = 8
CELLS = 27
MACRO_ITERS = 8
MICRO_MAX = 12
LANE_TAKE = True
MICRO_MIN = 6
VMEM = 67_043_328
EARLY = 8
LEAD = 12
ROW_COL = ("row_0", "row_1", "col_0", "col_1")
ROW = ("row_0", "row_1")
COL = ("col_0", "col_1")
NEX = 8
NEY = 32
DEVICES = NEX * NEY


def block_order():
    yi, zi, yb, zb = np.meshgrid(np.arange(3), np.arange(3), np.arange(8), np.arange(8), indexing="ij")
    return ((3 * yb + yi) * VOX + 3 * zb + zi).reshape(-1)


def block_matrices():
    order = block_order()
    into = np.zeros((YZ, YZ), np.float32)
    into[order, np.arange(YZ)] = 1.0
    back = np.zeros((640, YZ), np.float32)
    back[np.arange(YZ), order] = 1.0
    return into, back


def at(xi, yi, zi):
    return xi * 9 + yi * 3 + zi


def helpers():
    lane = lax.broadcasted_iota(jnp.int32, (8, 128), 1)
    sub = lax.broadcasted_iota(jnp.int32, (8, 128), 0)
    low = lane < 64
    high_part, yb, zb = lane & 64, (lane >> 3) & 7, lane & 7
    y_part, z_part = lane & 56, lane & 7
    y_next = high_part | ((y_part + 8) & 56) | z_part
    y_prev = high_part | ((y_part + 56) & 56) | z_part
    z_next = high_part | y_part | ((z_part + 1) & 7)
    z_prev = high_part | y_part | ((z_part + 7) & 7)

    def taken(v, index):
        return jnp.take_along_axis(v, index, axis=1, mode="promise_in_bounds")

    if LANE_TAKE:
        ahead = (
            lambda v: pltpu.roll(v, 7, 0),
            lambda v: taken(v, y_next),
            lambda v: taken(v, z_next),
        )
        before = (
            lambda v: pltpu.roll(v, 1, 0),
            lambda v: taken(v, y_prev),
            lambda v: taken(v, z_prev),
        )
    else:
        ahead = (
            lambda v: pltpu.roll(v, 7, 0),
            lambda v: jnp.where(yb == 7, pltpu.roll(v, 56, 1), pltpu.roll(v, 120, 1)),
            lambda v: jnp.where(zb == 7, pltpu.roll(v, 7, 1), pltpu.roll(v, 127, 1)),
        )
        before = (
            lambda v: pltpu.roll(v, 1, 0),
            lambda v: jnp.where(yb == 0, pltpu.roll(v, 72, 1), pltpu.roll(v, 8, 1)),
            lambda v: jnp.where(zb == 0, pltpu.roll(v, 121, 1), pltpu.roll(v, 1, 1)),
        )

    def both_halves(acc):
        acc = acc + pltpu.roll(acc, 4, 0)
        acc = acc + pltpu.roll(acc, 2, 0)
        acc = acc + pltpu.roll(acc, 1, 0)
        first = jnp.sum(jnp.where(low, acc, 0.0), axis=1, keepdims=True)
        second = jnp.sum(jnp.where(low, 0.0, acc), axis=1, keepdims=True)
        return first, second

    def total(acc):
        first, second = both_halves(acc)
        return jnp.where(low, first, second)

    return lane, sub, low, ahead, before, both_halves, total


def coords(cell):
    return cell // 9, (cell // 3) % 3, cell % 3


def side(cell, axis):
    xi, yi, zi = coords(cell)
    return (yi * 3 + zi, xi * 3 + zi, xi * 3 + yi)[axis]


def moved(cell, axis, step):
    spot = list(coords(cell))
    spot[axis] += step
    return at(*spot)


def cells_kernel(
    cond_hbm,
    count_hbm,
    current_hbm,
    load_hbm,
    phase_hbm,
    grain_hbm,
    into_hbm,
    path_hbm,
    steps_hbm,
    sums_hbm,
    packed_hbm,
    path,
    steps,
    sums,
    packed_ref,
    cond_ref,
    count_ref,
    current_ref,
    load_ref,
    phase_ref,
    grain_ref,
    into_ref,
    native,
    face,
    res,
    way,
    img,
    halo,
    alphas,
    betas,
    norms,
    energy,
    partial,
    sems,
    path_sems,
):
    f32 = jnp.float32
    copies = [
        pltpu.make_async_copy(src, dst, sems.at[n])
        for n, (src, dst) in enumerate(
            (
                (phase_hbm, phase_ref),
                (grain_hbm, grain_ref),
                (into_hbm, into_ref),
                (cond_hbm, cond_ref),
                (count_hbm, count_ref),
                (current_hbm, current_ref),
                (load_hbm, load_ref),
            )
        )
    ]
    for copy in copies:
        copy.start()
    lane, sub, low, ahead, before, both_halves, total = helpers()
    zero = jnp.zeros((8, 128), f32)
    for copy in copies:
        copy.wait()

    phase = phase_ref[...]
    conduct = jnp.where(phase == 0, cond_ref[0], jnp.where(phase == 1, cond_ref[1], cond_ref[2])) * grain_ref[...]
    part_a = conduct.astype(jnp.bfloat16)
    rest = conduct - part_a.astype(f32)
    part_b = rest.astype(jnp.bfloat16)
    part_c = (rest - part_b.astype(f32)).astype(jnp.bfloat16)
    into = into_ref[...]
    ordered = jnp.dot(jnp.concatenate([part_a, part_b, part_c], axis=0), into, preferred_element_type=f32)
    ordered = ordered[0:192] + ordered[192:384] + ordered[384:576]
    for t in range(4):
        native[t] = ordered[:, t * 128 : (t + 1) * 128]
    native[4, :, 0:64] = ordered[:, 512:576]

    for pair in range(4):
        cells = []
        for xi in range(3):
            for g in range(9):
                first = native[g // 2, pl.ds(2 * pair * VOX + xi, 8, stride=3), :]
                second = native[g // 2, pl.ds((2 * pair + 1) * VOX + xi, 8, stride=3), :]
                if g % 2 == 0:
                    cells.append(jnp.where(low, first, pltpu.roll(second, 64, 1)))
                else:
                    cells.append(jnp.where(low, pltpu.roll(first, 64, 1), second))
        for axis in range(3):
            faces = []
            acc_face = None
            for cell in range(CELLS):
                if coords(cell)[axis] < 2:
                    nxt = cells[moved(cell, axis, 1)]
                else:
                    nxt = ahead[axis](cells[moved(cell, axis, -2)])
                value = (cells[cell] + nxt) * 0.5
                faces.append(value)
                face[pair, axis, cell] = value
                acc_face = value if acc_face is None else acc_face + value
            acc = None
            for cell in range(CELLS):
                if coords(cell)[axis] > 0:
                    back = faces[moved(cell, axis, -1)]
                else:
                    back = before[axis](faces[moved(cell, axis, 2)])
                value = faces[cell] - back
                res[pair, axis, cell] = value
                way[pair, axis, cell] = value
                path[0, pair, axis, cell] = value
                acc = value * value if acc is None else acc + value * value
            norms[pair, axis] = total(acc)
            sums[pair, axis] = total(acc_face)
            energy[pair, axis] = zero

    most = count_ref[0]
    for e in range(1, DEPTH):
        most = jnp.maximum(most, count_ref[e])

    sums_copy = pltpu.make_async_copy(sums, sums_hbm, sems.at[8])
    sums_copy.start()

    def path_copy(k):
        return pltpu.make_async_copy(path.at[k], path_hbm.at[k], path_sems.at[k])

    path_copy(0).start()
    chains = [(pair, c) for pair in range(4) for c in range(3)]
    late = chains[EARLY:]

    def active(pair, k):
        return jnp.where(low, count_ref[2 * pair], count_ref[2 * pair + 1]) > k

    def set_step(pair, c, k, curve):
        norm = norms[pair, c]
        alpha = jnp.where(active(pair, k), norm / curve, 0.0)
        alphas[pair, c] = alpha
        steps[k, pair, c] = alpha
        energy[pair, c] = energy[pair, c] + alpha * norm

    def far_fluxes(pair, c):
        for axis in range(3):
            for cell in range(CELLS):
                if coords(cell)[axis] == 2:
                    nxt = ahead[axis](way[pair, c, moved(cell, axis, -2)])
                    halo[pair, c, 2 * axis, side(cell, axis)] = face[pair, axis, cell] * (way[pair, c, cell] - nxt)

    def near_fluxes(pair, c):
        for axis in range(3):
            for spot in range(9):
                halo[pair, c, 2 * axis + 1, spot] = before[axis](halo[pair, c, 2 * axis, spot])

    def images(k):
        for pair, c in chains:
            flow = {}
            acc = None
            for cell in range(CELLS):
                here = way[pair, c, cell]
                out = None
                for axis in range(3):
                    spot = coords(cell)[axis]
                    if spot < 2:
                        flux = face[pair, axis, cell] * (here - way[pair, c, moved(cell, axis, 1)])
                    else:
                        flux = halo[pair, c, 2 * axis, side(cell, axis)]
                    if spot > 0:
                        back = flow.pop((axis, moved(cell, axis, -1)))
                    else:
                        back = halo[pair, c, 2 * axis + 1, side(cell, axis)]
                    if spot < 2:
                        flow[axis, cell] = flux
                    out = flux - back if out is None else out + (flux - back)
                img[pair, c, cell] = out
                acc = here * out if acc is None else acc + here * out
            if (pair, c) in late:
                partial[pair, c] = acc
            else:
                set_step(pair, c, k, total(acc))

    def finish(k):
        for pair, c in late:
            set_step(pair, c, k, total(partial[pair, c]))

    for n, chain in enumerate(chains):
        far_fluxes(*chain)
        if n >= LEAD:
            near_fluxes(*chains[n - LEAD])
    for chain in chains[len(chains) - LEAD :]:
        near_fluxes(*chain)
    images(0)

    def sweep(k, carry):
        finish(k - 1)
        for pair, c in chains:
            alpha = alphas[pair, c]
            acc = None
            for cell in range(CELLS):
                value = res[pair, c, cell] - alpha * img[pair, c, cell]
                res[pair, c, cell] = value
                acc = value * value if acc is None else acc + value * value
            new = total(acc)
            betas[pair, c] = jnp.where(active(pair, k), new / norms[pair, c], 0.0)
            norms[pair, c] = new
        for n, (pair, c) in enumerate(chains):
            beta = betas[pair, c]
            for cell in range(CELLS):
                value = res[pair, c, cell] + beta * way[pair, c, cell]
                way[pair, c, cell] = value
                path[k, pair, c, cell] = value
            far_fluxes(pair, c)
            if n >= LEAD:
                near_fluxes(*chains[n - LEAD])
        path_copy(k).start()
        for chain in chains[len(chains) - LEAD :]:
            near_fluxes(*chain)
        images(k)
        return carry

    lax.fori_loop(1, most, sweep, 0)
    finish(most - 1)
    steps_copy = pltpu.make_async_copy(steps, steps_hbm, sems.at[9])
    steps_copy.start()

    share = 1.0 / (VOX * YZ)
    packed = zero
    for pair in range(4):
        for d in range(3):
            value = (sums[pair, d] - energy[pair, d]) * share
            packed = jnp.where(lane == d * DEPTH + 2 * pair, value, packed)
            packed = jnp.where(lane == d * DEPTH + 2 * pair + 1, pltpu.roll(value, 64, 1), packed)
    for e in range(DEPTH):
        packed = jnp.where(lane == 3 * DEPTH + e, current_ref[e], packed)
        packed = jnp.where(lane == 4 * DEPTH + e, load_ref[e], packed)
    for block in range(DEVICES // 8):
        packed_ref[block * 8 : block * 8 + 8, :] = packed
    packed_copy = pltpu.make_async_copy(packed_ref, packed_hbm, sems.at[10])
    packed_copy.start()

    def settle(k, carry):
        path_copy(k).wait()
        return carry

    lax.fori_loop(0, most, settle, 0)
    sums_copy.wait()
    steps_copy.wait()
    packed_copy.wait()


def output_kernel(
    count_hbm,
    path_hbm,
    steps_hbm,
    sums_hbm,
    back_hbm,
    states_hbm,
    tangent_ref,
    count_ref,
    path,
    steps,
    sums,
    back_ref,
    blocked,
    states_ref,
    sems,
    path_sems,
):
    f32 = jnp.float32
    count_copy = pltpu.make_async_copy(count_hbm, count_ref, sems.at[0])
    count_copy.start()

    def path_copy(pair, k):
        return pltpu.make_async_copy(path_hbm.at[k, pair], path.at[k, pair], path_sems.at[pair, k])

    for k in range(MICRO_MIN):
        path_copy(0, k).start()
    copies = [
        pltpu.make_async_copy(steps_hbm, steps, sems.at[1]),
        pltpu.make_async_copy(sums_hbm, sums, sems.at[2]),
        pltpu.make_async_copy(back_hbm, back_ref, sems.at[3]),
    ]
    for copy in copies:
        copy.start()
    lane, sub, low, ahead, before, both_halves, total = helpers()
    zero = jnp.zeros((8, 128), f32)
    count_copy.wait()
    most = count_ref[0]
    for e in range(1, DEPTH):
        most = jnp.maximum(most, count_ref[e])

    def begin(pair, k, carry):
        path_copy(pair, k).start()
        return carry

    lax.fori_loop(MICRO_MIN, most, functools.partial(begin, 0), 0)
    for pair in range(1, 4):
        lax.fori_loop(0, most, functools.partial(begin, pair), 0)
    for copy in copies:
        copy.wait()

    share = 1.0 / (VOX * YZ)
    row_e = lax.broadcasted_iota(jnp.int32, (16, 128), 1)
    row_d = lax.broadcasted_iota(jnp.int32, (16, 128), 0)
    tangent = jnp.zeros((16, 128), f32)
    rows = 2 * 3 * VOX
    states_copies = []
    for pair in range(4):
        for c in range(3):

            def add(k, held):
                if c == 0:
                    path_copy(pair, k).wait()
                alpha = steps[k, pair, c]
                return tuple(value + alpha * path[k, pair, c, cell] for cell, value in enumerate(held))

            held = lax.fori_loop(0, most, add, (zero,) * CELLS)
            accs = [None] * 3
            for cell in range(CELLS):
                for d in range(3):
                    term = held[cell] * path[0, pair, d, cell]
                    accs[d] = term if accs[d] is None else accs[d] + term
            for xi in range(3):
                row = held[xi * 9 : xi * 9 + 9]
                start = c * VOX + xi
                for t in range(5):
                    if t < 4:
                        one = jnp.where(low, row[2 * t], pltpu.roll(row[2 * t + 1], 64, 1))
                        two = jnp.where(low, pltpu.roll(row[2 * t], 64, 1), row[2 * t + 1])
                    else:
                        one = jnp.where(low, row[8], 0.0)
                        two = jnp.where(low, pltpu.roll(row[8], 64, 1), 0.0)
                    blocked[t, pl.ds(start, 8, stride=3), :] = one
                    blocked[t, pl.ds(start + 3 * VOX, 8, stride=3), :] = two
            for d in range(3):
                value = total(accs[d])
                value = (sums[pair, d] - value if d == c else -value) * share
                for half in range(2):
                    flat = value[0:1, 64 * half : 64 * half + 1]
                    tangent = jnp.where((row_d == 3 * d + c) & (row_e == 2 * pair + half), flat, tangent)
        lhs = jnp.concatenate([blocked[t] for t in range(5)], axis=1)
        upper = lhs.astype(jnp.bfloat16)
        lower = (lhs - upper.astype(f32)).astype(jnp.bfloat16)
        both = jnp.dot(jnp.concatenate([upper, lower], axis=0), back_ref[...], preferred_element_type=f32)
        place = pl.ds(pair * rows, rows)
        states_ref[place, :] = both[:rows] + both[rows:]
        states_copies.append(pltpu.make_async_copy(states_ref.at[place], states_hbm.at[place], sems.at[4 + pair]))
        states_copies[pair].start()
    for n in range(9):
        tangent_ref[n] = tangent[n : n + 1, 0:DEPTH]
    for copy in states_copies:
        copy.wait()


def solve_cells(phases, grain, phase_cond, counts, current, load):
    into, back = block_matrices()
    f32 = jnp.float32
    hbm = pl.BlockSpec(memory_space=pltpu.HBM)
    vmem = pl.BlockSpec(memory_space=pltpu.VMEM)
    field = pltpu.VMEM((4, 3, CELLS, 8, 128), f32)
    chain = pltpu.VMEM((4, 3, 8, 128), f32)
    path, steps, sums, packed = pl.pallas_call(
        cells_kernel,
        out_shape=(
            jax.ShapeDtypeStruct((MICRO_MAX, 4, 3, CELLS, 8, 128), f32),
            jax.ShapeDtypeStruct((MICRO_MAX, 4, 3, 8, 128), f32),
            jax.ShapeDtypeStruct((4, 3, 8, 128), f32),
            jax.ShapeDtypeStruct((DEVICES, 128), f32),
        ),
        in_specs=[hbm] * 7,
        out_specs=(hbm,) * 4,
        scratch_shapes=[
            pltpu.VMEM((MICRO_MAX, 4, 3, CELLS, 8, 128), f32),
            pltpu.VMEM((MICRO_MAX, 4, 3, 8, 128), f32),
            chain,
            pltpu.VMEM((DEVICES, 128), f32),
            pltpu.SMEM((3,), f32),
            pltpu.SMEM((DEPTH,), jnp.int32),
            pltpu.SMEM((DEPTH,), f32),
            pltpu.SMEM((DEPTH,), f32),
            pltpu.VMEM((DEPTH * VOX, YZ), jnp.int32),
            pltpu.VMEM((DEPTH * VOX, YZ), f32),
            pltpu.VMEM((YZ, YZ), jnp.bfloat16),
            pltpu.VMEM((5, DEPTH * VOX, 128), f32),
            field,
            field,
            field,
            field,
            pltpu.VMEM((4, 3, 6, 9, 8, 128), f32),
            chain,
            chain,
            chain,
            chain,
            chain,
            pltpu.SemaphoreType.DMA((11,)),
            pltpu.SemaphoreType.DMA((MICRO_MAX,)),
        ],
        compiler_params=pltpu.CompilerParams(vmem_limit_bytes=VMEM),
        name="cells",
    )(phase_cond, counts, current, load, phases, grain, jnp.asarray(into, jnp.bfloat16))

    def output():
        return pl.pallas_call(
            output_kernel,
            out_shape=(
                jax.ShapeDtypeStruct((DEPTH * 3 * VOX, YZ), f32),
                jax.ShapeDtypeStruct((9, 1, DEPTH), f32),
            ),
            in_specs=[hbm] * 5,
            out_specs=(hbm, vmem),
            scratch_shapes=[
                pltpu.SMEM((DEPTH,), jnp.int32),
                pltpu.VMEM((MICRO_MAX, 4, 3, CELLS, 8, 128), f32),
                pltpu.VMEM((MICRO_MAX, 4, 3, 8, 128), f32),
                chain,
                pltpu.VMEM((640, YZ), jnp.bfloat16),
                pltpu.VMEM((5, 2 * 3 * VOX, 128), f32),
                pltpu.VMEM((DEPTH * 3 * VOX, YZ), f32),
                pltpu.SemaphoreType.DMA((8,)),
                pltpu.SemaphoreType.DMA((4, MICRO_MAX)),
            ],
            compiler_params=pltpu.CompilerParams(vmem_limit_bytes=VMEM),
            cost_estimate=pl.CostEstimate(flops=400_000_000, bytes_accessed=4_000_000, transcendentals=0),
            name="output",
        )(counts, path, steps, sums, jnp.asarray(back, jnp.bfloat16))

    return packed, output


def coarse_kernel(place_ref, packed_ref, increment_ref, residual_ref):
    f32 = jnp.float32
    nodes = packed_ref[...].T
    shape = (DEPTH, DEVICES)
    lane = lax.broadcasted_iota(jnp.int32, shape, 1)
    sub = lax.broadcasted_iota(jnp.int32, shape, 0)
    col, row = lane & (NEY - 1), lane >> 5
    has_next = (row < NEX - 1, col < NEY - 1, sub < DEPTH - 1)
    has_back = (row > 0, col > 0, sub > 0)

    def following(v, axis):
        if axis == 2:
            return pltpu.roll(v, DEPTH - 1, 0)
        return pltpu.roll(v, DEVICES - (NEY if axis == 0 else 1), 1)

    def preceding(v, axis):
        if axis == 2:
            return pltpu.roll(v, 1, 0)
        return pltpu.roll(v, NEY if axis == 0 else 1, 1)

    def total(v):
        v = v[:, :128] + v[:, 128:]
        v = v + pltpu.roll(v, 4, 0)
        v = v + pltpu.roll(v, 2, 0)
        v = v + pltpu.roll(v, 1, 0)
        return jnp.sum(v, axis=1, keepdims=True)

    own = None
    links = []
    for axis in range(3):
        k = nodes[axis * DEPTH : (axis + 1) * DEPTH]
        for shift, inside in ((following, has_next[axis]), (preceding, has_back[axis])):
            other = jnp.where(inside, shift(k, axis), 0.0)
            mean = 0.5 * (k + other)
            own = mean if own is None else own + mean
            links.append((shift, axis, jnp.where(inside, mean, 0.0)))

    def apply(v):
        out = own * v
        for shift, axis, weight in links:
            out = out - weight * shift(v, axis)
        return out

    current = nodes[3 * DEPTH : 4 * DEPTH]
    residual = nodes[4 * DEPTH : 5 * DEPTH] - apply(current)
    increment = direction = trail = norm = step = None
    for iteration in range(MACRO_ITERS):
        image = apply(residual)
        new, curve = total(residual * residual), total(residual * image)
        if iteration == 0:
            step = new / curve
            direction, trail = residual, image
            increment = step * direction
        else:
            ratio = new / norm
            step = new / (curve - ratio * (new / step))
            direction = residual + ratio * direction
            trail = image + ratio * trail
            increment = increment + step * direction
        residual = residual - step * trail
        norm = new

    spot = sub[:, :128] == lane[:, :128]
    for value, ref in ((increment, increment_ref), (residual, residual_ref)):
        column = jnp.sum(jnp.where(lane == place_ref[0], value, 0.0), axis=1, keepdims=True)
        line = jnp.sum(jnp.where(spot, column, 0.0), axis=0, keepdims=True)
        ref[...] = line[:, :DEPTH]


def solve_coarse(place, packed):
    smem = pl.BlockSpec(memory_space=pltpu.SMEM)
    vmem = pl.BlockSpec(memory_space=pltpu.VMEM)
    line = jax.ShapeDtypeStruct((1, DEPTH), jnp.float32)
    return pl.pallas_call(
        coarse_kernel,
        out_shape=(line, line),
        in_specs=[smem, vmem],
        out_specs=(vmem, vmem),
        compiler_params=pltpu.CompilerParams(vmem_limit_bytes=4 * 1024 * 1024),
        name="coarse",
    )(place, packed)


def shards(phases, grain, phase_cond, micro_counts, current, load):
    packed, output = solve_cells(
        phases.reshape(DEPTH * VOX, YZ),
        grain.reshape(DEPTH * VOX, YZ),
        phase_cond,
        micro_counts.reshape(DEPTH),
        current.reshape(DEPTH),
        load.reshape(DEPTH),
    )
    whole = lax.all_to_all(packed.reshape(DEVICES, 1, 128), ROW_COL, 0, 0, tiled=True)
    states, tangent = output()
    place = lax.axis_index(ROW_COL).astype(jnp.int32).reshape(1)
    increment, residual = solve_coarse(place, whole.reshape(DEVICES, 128))
    return (
        states.reshape(1, 1, DEPTH, 3, VOX, YZ),
        tangent.reshape(3, 3, 1, 1, DEPTH).transpose(2, 3, 4, 0, 1),
        increment.reshape(1, 1, DEPTH),
        residual.reshape(1, 1, DEPTH),
    )


def solution(mesh):
    torus = Mesh(mesh.devices.reshape(4, 2, 4, 8), ("row_0", "row_1", "col_0", "col_1"))
    in_specs = (
        P(ROW, COL, None, None, None),
        P(ROW, COL, None, None, None),
        P(),
        P(ROW, COL, None),
        P(ROW, COL, None),
        P(ROW, COL, None),
    )
    out_specs = (
        P(ROW, COL, None, None, None, None),
        P(ROW, COL, None, None, None),
        P(ROW, COL, None),
        P(ROW, COL, None),
    )
    return jax.shard_map(
        shards, mesh=torus, in_specs=in_specs, out_specs=out_specs, check_vma=False
    )
```

```python
import functools

import jax
import jax.numpy as jnp
import numpy as np
from jax import lax
from jax.experimental import pallas as pl
from jax.experimental.pallas import tpu as pltpu
from jax.sharding import Mesh
from jax.sharding import PartitionSpec as P

VOX = 24
YZ = 576
DEPTH = 8
CELLS = 27
MACRO_ITERS = 8
MICRO_MAX = 12
LANE_TAKE = True
MICRO_MIN = 6
VMEM = 67_043_328
ROOM = 400 * 1024
EARLY = 8
LEAD = 12
ROW_COL = ("row_0", "row_1", "col_0", "col_1")
ROW = ("row_0", "row_1")
COL = ("col_0", "col_1")
NEX = 8
NEY = 32
DEVICES = NEX * NEY


def block_order():
    yi, zi, yb, zb = np.meshgrid(np.arange(3), np.arange(3), np.arange(8), np.arange(8), indexing="ij")
    return ((3 * yb + yi) * VOX + 3 * zb + zi).reshape(-1)


def block_matrices():
    order = block_order()
    into = np.zeros((YZ, YZ), np.float32)
    into[order, np.arange(YZ)] = 1.0
    back = np.zeros((640, YZ), np.float32)
    back[np.arange(YZ), order] = 1.0
    return into, back


def at(xi, yi, zi):
    return xi * 9 + yi * 3 + zi


def helpers():
    lane = lax.broadcasted_iota(jnp.int32, (8, 128), 1)
    sub = lax.broadcasted_iota(jnp.int32, (8, 128), 0)
    low = lane < 64
    high_part, yb, zb = lane & 64, (lane >> 3) & 7, lane & 7
    y_part, z_part = lane & 56, lane & 7
    y_next = high_part | ((y_part + 8) & 56) | z_part
    y_prev = high_part | ((y_part + 56) & 56) | z_part
    z_next = high_part | y_part | ((z_part + 1) & 7)
    z_prev = high_part | y_part | ((z_part + 7) & 7)

    def taken(v, index):
        return jnp.take_along_axis(v, index, axis=1, mode="promise_in_bounds")

    if LANE_TAKE:
        ahead = (
            lambda v: pltpu.roll(v, 7, 0),
            lambda v: taken(v, y_next),
            lambda v: taken(v, z_next),
        )
        before = (
            lambda v: pltpu.roll(v, 1, 0),
            lambda v: taken(v, y_prev),
            lambda v: taken(v, z_prev),
        )
    else:
        ahead = (
            lambda v: pltpu.roll(v, 7, 0),
            lambda v: jnp.where(yb == 7, pltpu.roll(v, 56, 1), pltpu.roll(v, 120, 1)),
            lambda v: jnp.where(zb == 7, pltpu.roll(v, 7, 1), pltpu.roll(v, 127, 1)),
        )
        before = (
            lambda v: pltpu.roll(v, 1, 0),
            lambda v: jnp.where(yb == 0, pltpu.roll(v, 72, 1), pltpu.roll(v, 8, 1)),
            lambda v: jnp.where(zb == 0, pltpu.roll(v, 121, 1), pltpu.roll(v, 1, 1)),
        )

    def both_halves(acc):
        acc = acc + pltpu.roll(acc, 4, 0)
        acc = acc + pltpu.roll(acc, 2, 0)
        acc = acc + pltpu.roll(acc, 1, 0)
        first = jnp.sum(jnp.where(low, acc, 0.0), axis=1, keepdims=True)
        second = jnp.sum(jnp.where(low, 0.0, acc), axis=1, keepdims=True)
        return first, second

    def total(acc):
        first, second = both_halves(acc)
        return jnp.where(low, first, second)

    return lane, sub, low, ahead, before, both_halves, total


def coords(cell):
    return cell // 9, (cell // 3) % 3, cell % 3


def side(cell, axis):
    xi, yi, zi = coords(cell)
    return (yi * 3 + zi, xi * 3 + zi, xi * 3 + yi)[axis]


def moved(cell, axis, step):
    spot = list(coords(cell))
    spot[axis] += step
    return at(*spot)


def cells_kernel(
    cond_hbm,
    count_hbm,
    current_hbm,
    load_hbm,
    phase_hbm,
    grain_hbm,
    into_hbm,
    path_hbm,
    steps_hbm,
    packed_hbm,
    path,
    steps,
    packed_ref,
    cond_ref,
    count_ref,
    current_ref,
    load_ref,
    phase_ref,
    grain_ref,
    into_ref,
    native,
    face,
    res,
    way,
    img,
    halo,
    alphas,
    betas,
    norms,
    energy,
    partial,
    sems,
    path_sems,
):
    f32 = jnp.float32
    copies = [
        pltpu.make_async_copy(src, dst, sems.at[n])
        for n, (src, dst) in enumerate(
            (
                (phase_hbm, phase_ref),
                (grain_hbm, grain_ref),
                (into_hbm, into_ref),
                (cond_hbm, cond_ref),
                (count_hbm, count_ref),
                (current_hbm, current_ref),
                (load_hbm, load_ref),
            )
        )
    ]
    for copy in copies:
        copy.start()
    lane, sub, low, ahead, before, both_halves, total = helpers()
    zero = jnp.zeros((8, 128), f32)
    for copy in copies:
        copy.wait()

    phase = phase_ref[...]
    conduct = jnp.where(phase == 0, cond_ref[0], jnp.where(phase == 1, cond_ref[1], cond_ref[2])) * grain_ref[...]
    part_a = conduct.astype(jnp.bfloat16)
    rest = conduct - part_a.astype(f32)
    part_b = rest.astype(jnp.bfloat16)
    part_c = (rest - part_b.astype(f32)).astype(jnp.bfloat16)
    into = into_ref[...]
    ordered = jnp.dot(jnp.concatenate([part_a, part_b, part_c], axis=0), into, preferred_element_type=f32)
    ordered = ordered[0:192] + ordered[192:384] + ordered[384:576]
    for t in range(4):
        native[t] = ordered[:, t * 128 : (t + 1) * 128]
    native[4, :, 0:64] = ordered[:, 512:576]

    for pair in range(4):
        cells = []
        for xi in range(3):
            for g in range(9):
                first = native[g // 2, pl.ds(2 * pair * VOX + xi, 8, stride=3), :]
                second = native[g // 2, pl.ds((2 * pair + 1) * VOX + xi, 8, stride=3), :]
                if g % 2 == 0:
                    cells.append(jnp.where(low, first, pltpu.roll(second, 64, 1)))
                else:
                    cells.append(jnp.where(low, pltpu.roll(first, 64, 1), second))
        for axis in range(3):
            faces = []
            acc_face = None
            for cell in range(CELLS):
                if coords(cell)[axis] < 2:
                    nxt = cells[moved(cell, axis, 1)]
                else:
                    nxt = ahead[axis](cells[moved(cell, axis, -2)])
                value = (cells[cell] + nxt) * 0.5
                faces.append(value)
                face[pair, axis, cell] = value
                acc_face = value if acc_face is None else acc_face + value
            acc = None
            for cell in range(CELLS):
                if coords(cell)[axis] > 0:
                    back = faces[moved(cell, axis, -1)]
                else:
                    back = before[axis](faces[moved(cell, axis, 2)])
                value = faces[cell] - back
                res[pair, axis, cell] = value
                way[pair, axis, cell] = value
                path[0, pair, axis, cell] = value
                acc = value * value if acc is None else acc + value * value
            norms[pair, axis] = total(acc)
            steps[MICRO_MAX, pair, axis] = total(acc_face)
            energy[pair, axis] = zero

    most = count_ref[0]
    for e in range(1, DEPTH):
        most = jnp.maximum(most, count_ref[e])
    steps[MICRO_MAX + 1, 0, 0] = jnp.full((8, 128), most, jnp.int32).astype(f32)


    def path_copy(k):
        return pltpu.make_async_copy(path.at[k], path_hbm.at[k], path_sems.at[k])

    path_copy(0).start()
    chains = [(pair, c) for pair in range(4) for c in range(3)]
    late = chains[EARLY:]

    def active(pair, k):
        return jnp.where(low, count_ref[2 * pair], count_ref[2 * pair + 1]) > k

    def set_step(pair, c, k, curve):
        norm = norms[pair, c]
        alpha = jnp.where(active(pair, k), norm / curve, 0.0)
        alphas[pair, c] = alpha
        steps[k, pair, c] = alpha
        energy[pair, c] = energy[pair, c] + alpha * norm

    def far_fluxes(pair, c):
        for axis in range(3):
            for cell in range(CELLS):
                if coords(cell)[axis] == 2:
                    nxt = ahead[axis](way[pair, c, moved(cell, axis, -2)])
                    halo[pair, c, 2 * axis, side(cell, axis)] = face[pair, axis, cell] * (way[pair, c, cell] - nxt)

    def near_fluxes(pair, c):
        for axis in range(3):
            for spot in range(9):
                halo[pair, c, 2 * axis + 1, spot] = before[axis](halo[pair, c, 2 * axis, spot])

    def images(k):
        for pair, c in chains:
            flow = {}
            acc = None
            for cell in range(CELLS):
                here = way[pair, c, cell]
                out = None
                for axis in range(3):
                    spot = coords(cell)[axis]
                    if spot < 2:
                        flux = face[pair, axis, cell] * (here - way[pair, c, moved(cell, axis, 1)])
                    else:
                        flux = halo[pair, c, 2 * axis, side(cell, axis)]
                    if spot > 0:
                        back = flow.pop((axis, moved(cell, axis, -1)))
                    else:
                        back = halo[pair, c, 2 * axis + 1, side(cell, axis)]
                    if spot < 2:
                        flow[axis, cell] = flux
                    out = flux - back if out is None else out + (flux - back)
                img[pair, c, cell] = out
                acc = here * out if acc is None else acc + here * out
            if (pair, c) in late:
                partial[pair, c] = acc
            else:
                set_step(pair, c, k, total(acc))

    def finish(k):
        for pair, c in late:
            set_step(pair, c, k, total(partial[pair, c]))

    for n, chain in enumerate(chains):
        far_fluxes(*chain)
        if n >= LEAD:
            near_fluxes(*chains[n - LEAD])
    for chain in chains[len(chains) - LEAD :]:
        near_fluxes(*chain)
    images(0)

    def sweep(k, carry):
        finish(k - 1)
        for pair, c in chains:
            alpha = alphas[pair, c]
            acc = None
            for cell in range(CELLS):
                value = res[pair, c, cell] - alpha * img[pair, c, cell]
                res[pair, c, cell] = value
                acc = value * value if acc is None else acc + value * value
            new = total(acc)
            betas[pair, c] = jnp.where(active(pair, k), new / norms[pair, c], 0.0)
            norms[pair, c] = new
        for n, (pair, c) in enumerate(chains):
            beta = betas[pair, c]
            for cell in range(CELLS):
                value = res[pair, c, cell] + beta * way[pair, c, cell]
                way[pair, c, cell] = value
                path[k, pair, c, cell] = value
            far_fluxes(pair, c)
            if n >= LEAD:
                near_fluxes(*chains[n - LEAD])
        path_copy(k).start()
        for chain in chains[len(chains) - LEAD :]:
            near_fluxes(*chain)
        images(k)
        return carry

    lax.fori_loop(1, most, sweep, 0)
    finish(most - 1)
    steps_copy = pltpu.make_async_copy(steps, steps_hbm, sems.at[9])
    steps_copy.start()

    share = 1.0 / (VOX * YZ)
    packed = zero
    for pair in range(4):
        for d in range(3):
            value = (steps[MICRO_MAX, pair, d] - energy[pair, d]) * share
            packed = jnp.where(lane == d * DEPTH + 2 * pair, value, packed)
            packed = jnp.where(lane == d * DEPTH + 2 * pair + 1, pltpu.roll(value, 64, 1), packed)
    for e in range(DEPTH):
        packed = jnp.where(lane == 3 * DEPTH + e, current_ref[e], packed)
        packed = jnp.where(lane == 4 * DEPTH + e, load_ref[e], packed)
    for block in range(DEVICES // 8):
        packed_ref[block * 8 : block * 8 + 8, :] = packed
    packed_copy = pltpu.make_async_copy(packed_ref, packed_hbm, sems.at[10])
    packed_copy.start()

    def settle(k, carry):
        path_copy(k).wait()
        return carry

    lax.fori_loop(0, most, settle, 0)
    steps_copy.wait()
    packed_copy.wait()


def output_kernel(
    path_hbm,
    steps_hbm,
    back_hbm,
    states_hbm,
    tangent_ref,
    path,
    steps,
    back_ref,
    blocked,
    states_ref,
    sems,
    path_sems,
):
    f32 = jnp.float32
    steps_copy = pltpu.make_async_copy(steps_hbm, steps, sems.at[0])
    steps_copy.start()

    def path_copy(pair, k):
        return pltpu.make_async_copy(path_hbm.at[k, pair], path.at[k, pair], path_sems.at[pair, k])

    for k in range(MICRO_MIN):
        path_copy(0, k).start()
    back_copy = pltpu.make_async_copy(back_hbm, back_ref, sems.at[1])
    back_copy.start()
    lane, sub, low, ahead, before, both_halves, total = helpers()
    steps_copy.wait()
    most = jnp.max(steps[MICRO_MAX + 1, 0, 0]).astype(jnp.int32)

    def begin(pair, k, carry):
        path_copy(pair, k).start()
        return carry

    lax.fori_loop(MICRO_MIN, most, functools.partial(begin, 0), 0)
    for pair in range(1, 4):
        lax.fori_loop(0, most, functools.partial(begin, pair), 0)
    back_copy.wait()

    share = 1.0 / (VOX * YZ)
    row_e = lax.broadcasted_iota(jnp.int32, (16, 128), 1)
    row_d = lax.broadcasted_iota(jnp.int32, (16, 128), 0)
    tangent = jnp.zeros((16, 128), f32)
    rows = 2 * 3 * VOX
    states_copies = []
    for pair in range(4):
        for c in range(3):

            def add(k, held):
                if c == 0:
                    path_copy(pair, k).wait()
                alpha = steps[k, pair, c]
                return tuple(value + alpha * path[k, pair, c, cell] for cell, value in enumerate(held))

            if c == 0:
                for k in range(MICRO_MIN):
                    path_copy(pair, k).wait()
            alpha = [steps[k, pair, c] for k in range(MICRO_MIN)]
            held = []
            for cell in range(CELLS):
                value = alpha[0] * path[0, pair, c, cell]
                for k in range(1, MICRO_MIN):
                    value = value + alpha[k] * path[k, pair, c, cell]
                held.append(value)
            held = lax.fori_loop(MICRO_MIN, most, add, tuple(held))
            accs = [None] * 3
            for cell in range(CELLS):
                for d in range(3):
                    term = held[cell] * path[0, pair, d, cell]
                    accs[d] = term if accs[d] is None else accs[d] + term
            for xi in range(3):
                row = held[xi * 9 : xi * 9 + 9]
                start = c * VOX + xi
                for t in range(5):
                    if t < 4:
                        one = jnp.where(low, row[2 * t], pltpu.roll(row[2 * t + 1], 64, 1))
                        two = jnp.where(low, pltpu.roll(row[2 * t], 64, 1), row[2 * t + 1])
                    else:
                        one = jnp.where(low, row[8], 0.0)
                        two = jnp.where(low, pltpu.roll(row[8], 64, 1), 0.0)
                    blocked[t, pl.ds(start, 8, stride=3), :] = one
                    blocked[t, pl.ds(start + 3 * VOX, 8, stride=3), :] = two
            for d in range(3):
                value = total(accs[d])
                value = (steps[MICRO_MAX, pair, d] - value if d == c else -value) * share
                for half in range(2):
                    flat = value[0:1, 64 * half : 64 * half + 1]
                    tangent = jnp.where((row_d == 3 * d + c) & (row_e == 2 * pair + half), flat, tangent)
        lhs = jnp.concatenate([blocked[t] for t in range(5)], axis=1)
        upper = lhs.astype(jnp.bfloat16)
        lower = (lhs - upper.astype(f32)).astype(jnp.bfloat16)
        both = jnp.dot(jnp.concatenate([upper, lower], axis=0), back_ref[...], preferred_element_type=f32)
        place = pl.ds(pair * rows, rows)
        states_ref[place, :] = both[:rows] + both[rows:]
        states_copies.append(pltpu.make_async_copy(states_ref.at[place], states_hbm.at[place], sems.at[2 + pair]))
        states_copies[pair].start()
    for n in range(9):
        tangent_ref[n] = tangent[n : n + 1, 0:DEPTH]
    for copy in states_copies:
        copy.wait()


def solve_cells(phases, grain, phase_cond, counts, current, load):
    into, back = block_matrices()
    f32 = jnp.float32
    hbm = pl.BlockSpec(memory_space=pltpu.HBM)
    vmem = pl.BlockSpec(memory_space=pltpu.VMEM)
    field = pltpu.VMEM((4, 3, CELLS, 8, 128), f32)
    chain = pltpu.VMEM((4, 3, 8, 128), f32)
    path, steps, packed = pl.pallas_call(
        cells_kernel,
        out_shape=(
            jax.ShapeDtypeStruct((MICRO_MAX, 4, 3, CELLS, 8, 128), f32),
            jax.ShapeDtypeStruct((MICRO_MAX + 2, 4, 3, 8, 128), f32),
            jax.ShapeDtypeStruct((DEVICES, 128), f32),
        ),
        in_specs=[hbm] * 7,
        out_specs=(hbm,) * 3,
        scratch_shapes=[
            pltpu.VMEM((MICRO_MAX, 4, 3, CELLS, 8, 128), f32),
            pltpu.VMEM((MICRO_MAX + 2, 4, 3, 8, 128), f32),
            pltpu.VMEM((DEVICES, 128), f32),
            pltpu.SMEM((3,), f32),
            pltpu.SMEM((DEPTH,), jnp.int32),
            pltpu.SMEM((DEPTH,), f32),
            pltpu.SMEM((DEPTH,), f32),
            pltpu.VMEM((DEPTH * VOX, YZ), jnp.int32),
            pltpu.VMEM((DEPTH * VOX, YZ), f32),
            pltpu.VMEM((YZ, YZ), jnp.bfloat16),
            pltpu.VMEM((5, DEPTH * VOX, 128), f32),
            field,
            field,
            field,
            field,
            pltpu.VMEM((4, 3, 6, 9, 8, 128), f32),
            chain,
            chain,
            chain,
            chain,
            chain,
            pltpu.SemaphoreType.DMA((11,)),
            pltpu.SemaphoreType.DMA((MICRO_MAX,)),
        ],
        compiler_params=pltpu.CompilerParams(vmem_limit_bytes=VMEM),
        name="cells",
    )(phase_cond, counts, current, load, phases, grain, jnp.asarray(into, jnp.bfloat16))

    def output():
        return pl.pallas_call(
            output_kernel,
            out_shape=(
                jax.ShapeDtypeStruct((DEPTH * 3 * VOX, YZ), f32),
                jax.ShapeDtypeStruct((9, 1, DEPTH), f32),
            ),
            in_specs=[hbm] * 3,
            out_specs=(hbm, vmem),
            scratch_shapes=[
                pltpu.VMEM((MICRO_MAX, 4, 3, CELLS, 8, 128), f32),
                pltpu.VMEM((MICRO_MAX + 2, 4, 3, 8, 128), f32),
                pltpu.VMEM((640, YZ), jnp.bfloat16),
                pltpu.VMEM((5, 2 * 3 * VOX, 128), f32),
                pltpu.VMEM((DEPTH * 3 * VOX, YZ), f32),
                pltpu.SemaphoreType.DMA((8,)),
                pltpu.SemaphoreType.DMA((4, MICRO_MAX)),
            ],
            compiler_params=pltpu.CompilerParams(vmem_limit_bytes=VMEM - ROOM),
            cost_estimate=pl.CostEstimate(flops=400_000_000, bytes_accessed=4_000_000, transcendentals=0),
            name="output",
        )(path, steps, jnp.asarray(back, jnp.bfloat16))

    return packed, output


def coarse_kernel(place_ref, packed_ref, increment_ref, residual_ref):
    f32 = jnp.float32
    nodes = packed_ref[...].T
    shape = (DEPTH, DEVICES)
    lane = lax.broadcasted_iota(jnp.int32, shape, 1)
    sub = lax.broadcasted_iota(jnp.int32, shape, 0)
    col, row = lane & (NEY - 1), lane >> 5
    has_next = (row < NEX - 1, col < NEY - 1, sub < DEPTH - 1)
    has_back = (row > 0, col > 0, sub > 0)

    def following(v, axis):
        if axis == 2:
            return pltpu.roll(v, DEPTH - 1, 0)
        return pltpu.roll(v, DEVICES - (NEY if axis == 0 else 1), 1)

    def preceding(v, axis):
        if axis == 2:
            return pltpu.roll(v, 1, 0)
        return pltpu.roll(v, NEY if axis == 0 else 1, 1)

    def total(v):
        v = v[:, :128] + v[:, 128:]
        v = v + pltpu.roll(v, 4, 0)
        v = v + pltpu.roll(v, 2, 0)
        v = v + pltpu.roll(v, 1, 0)
        return jnp.sum(v, axis=1, keepdims=True)

    own = None
    links = []
    for axis in range(3):
        k = nodes[axis * DEPTH : (axis + 1) * DEPTH]
        for shift, inside in ((following, has_next[axis]), (preceding, has_back[axis])):
            other = jnp.where(inside, shift(k, axis), 0.0)
            mean = 0.5 * (k + other)
            own = mean if own is None else own + mean
            links.append((shift, axis, jnp.where(inside, mean, 0.0)))

    def apply(v):
        out = own * v
        for shift, axis, weight in links:
            out = out - weight * shift(v, axis)
        return out

    current = nodes[3 * DEPTH : 4 * DEPTH]
    residual = nodes[4 * DEPTH : 5 * DEPTH] - apply(current)
    increment = direction = trail = norm = step = None
    for iteration in range(MACRO_ITERS):
        image = apply(residual)
        new, curve = total(residual * residual), total(residual * image)
        if iteration == 0:
            step = new / curve
            direction, trail = residual, image
            increment = step * direction
        else:
            ratio = new / norm
            step = new / (curve - ratio * (new / step))
            direction = residual + ratio * direction
            trail = image + ratio * trail
            increment = increment + step * direction
        residual = residual - step * trail
        norm = new

    spot = sub[:, :128] == lane[:, :128]
    for value, ref in ((increment, increment_ref), (residual, residual_ref)):
        column = jnp.sum(jnp.where(lane == place_ref[0], value, 0.0), axis=1, keepdims=True)
        line = jnp.sum(jnp.where(spot, column, 0.0), axis=0, keepdims=True)
        ref[...] = line[:, :DEPTH]


def solve_coarse(place, packed):
    smem = pl.BlockSpec(memory_space=pltpu.SMEM)
    vmem = pl.BlockSpec(memory_space=pltpu.VMEM)
    line = jax.ShapeDtypeStruct((1, DEPTH), jnp.float32)
    return pl.pallas_call(
        coarse_kernel,
        out_shape=(line, line),
        in_specs=[smem, vmem],
        out_specs=(vmem, vmem),
        compiler_params=pltpu.CompilerParams(vmem_limit_bytes=4 * 1024 * 1024),
        name="coarse",
    )(place, packed)


def shards(phases, grain, phase_cond, micro_counts, current, load):
    packed, output = solve_cells(
        phases.reshape(DEPTH * VOX, YZ),
        grain.reshape(DEPTH * VOX, YZ),
        phase_cond,
        micro_counts.reshape(DEPTH),
        current.reshape(DEPTH),
        load.reshape(DEPTH),
    )
    whole = lax.all_to_all(packed.reshape(DEVICES, 1, 128), ROW_COL, 0, 0, tiled=True)
    states, tangent = output()
    place = lax.axis_index(ROW_COL).astype(jnp.int32).reshape(1)
    increment, residual = solve_coarse(place, whole.reshape(DEVICES, 128))
    return (
        states.reshape(1, 1, DEPTH, 3, VOX, YZ),
        tangent.reshape(3, 3, 1, 1, DEPTH).transpose(2, 3, 4, 0, 1),
        increment.reshape(1, 1, DEPTH),
        residual.reshape(1, 1, DEPTH),
    )


def solution(mesh):
    torus = Mesh(mesh.devices.reshape(4, 2, 4, 8), ("row_0", "row_1", "col_0", "col_1"))
    in_specs = (
        P(ROW, COL, None, None, None),
        P(ROW, COL, None, None, None),
        P(),
        P(ROW, COL, None),
        P(ROW, COL, None),
        P(ROW, COL, None),
    )
    out_specs = (
        P(ROW, COL, None, None, None, None),
        P(ROW, COL, None, None, None),
        P(ROW, COL, None),
        P(ROW, COL, None),
    )
    return jax.shard_map(
        shards, mesh=torus, in_specs=in_specs, out_specs=out_specs, check_vma=False
    )
```

```python
import functools

import jax
import jax.numpy as jnp
import numpy as np
from jax import lax
from jax.experimental import pallas as pl
from jax.experimental.pallas import tpu as pltpu
from jax.sharding import Mesh
from jax.sharding import PartitionSpec as P

VOX = 24
YZ = 576
DEPTH = 8
CELLS = 27
MACRO_ITERS = 8
MICRO_MAX = 12
LANE_TAKE = True
MICRO_MIN = 6
VMEM = 67_043_328
ROOM = 400 * 1024
EARLY = 6
LEAD = 12
ROW_COL = ("row_0", "row_1", "col_0", "col_1")
ROW = ("row_0", "row_1")
COL = ("col_0", "col_1")
NEX = 8
NEY = 32
DEVICES = NEX * NEY


def block_order():
    yi, zi, yb, zb = np.meshgrid(np.arange(3), np.arange(3), np.arange(8), np.arange(8), indexing="ij")
    return ((3 * yb + yi) * VOX + 3 * zb + zi).reshape(-1)


def block_matrices():
    order = block_order()
    into = np.zeros((YZ, YZ), np.float32)
    into[order, np.arange(YZ)] = 1.0
    back = np.zeros((640, YZ), np.float32)
    back[np.arange(YZ), order] = 1.0
    return into, back


def at(xi, yi, zi):
    return xi * 9 + yi * 3 + zi


def helpers():
    lane = lax.broadcasted_iota(jnp.int32, (8, 128), 1)
    sub = lax.broadcasted_iota(jnp.int32, (8, 128), 0)
    low = lane < 64
    high_part, yb, zb = lane & 64, (lane >> 3) & 7, lane & 7
    y_part, z_part = lane & 56, lane & 7
    y_next = high_part | ((y_part + 8) & 56) | z_part
    y_prev = high_part | ((y_part + 56) & 56) | z_part
    z_next = high_part | y_part | ((z_part + 1) & 7)
    z_prev = high_part | y_part | ((z_part + 7) & 7)

    def taken(v, index):
        return jnp.take_along_axis(v, index, axis=1, mode="promise_in_bounds")

    if LANE_TAKE:
        ahead = (
            lambda v: pltpu.roll(v, 7, 0),
            lambda v: taken(v, y_next),
            lambda v: taken(v, z_next),
        )
        before = (
            lambda v: pltpu.roll(v, 1, 0),
            lambda v: taken(v, y_prev),
            lambda v: taken(v, z_prev),
        )
    else:
        ahead = (
            lambda v: pltpu.roll(v, 7, 0),
            lambda v: jnp.where(yb == 7, pltpu.roll(v, 56, 1), pltpu.roll(v, 120, 1)),
            lambda v: jnp.where(zb == 7, pltpu.roll(v, 7, 1), pltpu.roll(v, 127, 1)),
        )
        before = (
            lambda v: pltpu.roll(v, 1, 0),
            lambda v: jnp.where(yb == 0, pltpu.roll(v, 72, 1), pltpu.roll(v, 8, 1)),
            lambda v: jnp.where(zb == 0, pltpu.roll(v, 121, 1), pltpu.roll(v, 1, 1)),
        )

    def both_halves(acc):
        acc = acc + pltpu.roll(acc, 4, 0)
        acc = acc + pltpu.roll(acc, 2, 0)
        acc = acc + pltpu.roll(acc, 1, 0)
        first = jnp.sum(jnp.where(low, acc, 0.0), axis=1, keepdims=True)
        second = jnp.sum(jnp.where(low, 0.0, acc), axis=1, keepdims=True)
        return first, second

    def total(acc):
        first, second = both_halves(acc)
        return jnp.where(low, first, second)

    return lane, sub, low, ahead, before, both_halves, total


def coords(cell):
    return cell // 9, (cell // 3) % 3, cell % 3


def side(cell, axis):
    xi, yi, zi = coords(cell)
    return (yi * 3 + zi, xi * 3 + zi, xi * 3 + yi)[axis]


def moved(cell, axis, step):
    spot = list(coords(cell))
    spot[axis] += step
    return at(*spot)


def cells_kernel(
    cond_hbm,
    count_hbm,
    current_hbm,
    load_hbm,
    phase_hbm,
    grain_hbm,
    into_hbm,
    path_hbm,
    steps_hbm,
    packed_hbm,
    path,
    steps,
    packed_ref,
    cond_ref,
    count_ref,
    current_ref,
    load_ref,
    phase_ref,
    grain_ref,
    into_ref,
    native,
    face,
    res,
    way,
    img,
    halo,
    alphas,
    betas,
    norms,
    energy,
    partial,
    sems,
    path_sems,
):
    f32 = jnp.float32
    copies = [
        pltpu.make_async_copy(src, dst, sems.at[n])
        for n, (src, dst) in enumerate(
            (
                (phase_hbm, phase_ref),
                (grain_hbm, grain_ref),
                (into_hbm, into_ref),
                (cond_hbm, cond_ref),
                (count_hbm, count_ref),
                (current_hbm, current_ref),
                (load_hbm, load_ref),
            )
        )
    ]
    for copy in copies:
        copy.start()
    lane, sub, low, ahead, before, both_halves, total = helpers()
    zero = jnp.zeros((8, 128), f32)
    for copy in copies:
        copy.wait()

    phase = phase_ref[...]
    conduct = jnp.where(phase == 0, cond_ref[0], jnp.where(phase == 1, cond_ref[1], cond_ref[2])) * grain_ref[...]
    part_a = conduct.astype(jnp.bfloat16)
    rest = conduct - part_a.astype(f32)
    part_b = rest.astype(jnp.bfloat16)
    part_c = (rest - part_b.astype(f32)).astype(jnp.bfloat16)
    into = into_ref[...]
    ordered = jnp.dot(jnp.concatenate([part_a, part_b, part_c], axis=0), into, preferred_element_type=f32)
    ordered = ordered[0:192] + ordered[192:384] + ordered[384:576]
    for t in range(4):
        native[t] = ordered[:, t * 128 : (t + 1) * 128]
    native[4, :, 0:64] = ordered[:, 512:576]

    for pair in range(4):
        cells = []
        for xi in range(3):
            for g in range(9):
                first = native[g // 2, pl.ds(2 * pair * VOX + xi, 8, stride=3), :]
                second = native[g // 2, pl.ds((2 * pair + 1) * VOX + xi, 8, stride=3), :]
                if g % 2 == 0:
                    cells.append(jnp.where(low, first, pltpu.roll(second, 64, 1)))
                else:
                    cells.append(jnp.where(low, pltpu.roll(first, 64, 1), second))
        for axis in range(3):
            faces = []
            acc_face = None
            for cell in range(CELLS):
                if coords(cell)[axis] < 2:
                    nxt = cells[moved(cell, axis, 1)]
                else:
                    nxt = ahead[axis](cells[moved(cell, axis, -2)])
                value = (cells[cell] + nxt) * 0.5
                faces.append(value)
                face[pair, axis, cell] = value
                acc_face = value if acc_face is None else acc_face + value
            acc = None
            for cell in range(CELLS):
                if coords(cell)[axis] > 0:
                    back = faces[moved(cell, axis, -1)]
                else:
                    back = before[axis](faces[moved(cell, axis, 2)])
                value = faces[cell] - back
                res[pair, axis, cell] = value
                way[pair, axis, cell] = value
                path[0, pair, axis, cell] = value
                acc = value * value if acc is None else acc + value * value
            norms[pair, axis] = total(acc)
            steps[MICRO_MAX, pair, axis] = total(acc_face)
            energy[pair, axis] = zero

    most = count_ref[0]
    for e in range(1, DEPTH):
        most = jnp.maximum(most, count_ref[e])
    steps[MICRO_MAX + 1, 0, 0] = jnp.full((8, 128), most, jnp.int32).astype(f32)


    def path_copy(k):
        return pltpu.make_async_copy(path.at[k], path_hbm.at[k], path_sems.at[k])

    path_copy(0).start()
    chains = [(pair, c) for pair in range(4) for c in range(3)]
    late = chains[EARLY:]

    def active(pair, k):
        return jnp.where(low, count_ref[2 * pair], count_ref[2 * pair + 1]) > k

    def set_step(pair, c, k, curve):
        norm = norms[pair, c]
        alpha = jnp.where(active(pair, k), norm / curve, 0.0)
        alphas[pair, c] = alpha
        steps[k, pair, c] = alpha
        energy[pair, c] = energy[pair, c] + alpha * norm

    def far_fluxes(pair, c):
        for axis in range(3):
            for cell in range(CELLS):
                if coords(cell)[axis] == 2:
                    nxt = ahead[axis](way[pair, c, moved(cell, axis, -2)])
                    halo[pair, c, 2 * axis, side(cell, axis)] = face[pair, axis, cell] * (way[pair, c, cell] - nxt)

    def near_fluxes(pair, c):
        for axis in range(3):
            for spot in range(9):
                halo[pair, c, 2 * axis + 1, spot] = before[axis](halo[pair, c, 2 * axis, spot])

    def images(k):
        for pair, c in chains:
            flow = {}
            acc = None
            for cell in range(CELLS):
                here = way[pair, c, cell]
                out = None
                for axis in range(3):
                    spot = coords(cell)[axis]
                    if spot < 2:
                        flux = face[pair, axis, cell] * (here - way[pair, c, moved(cell, axis, 1)])
                    else:
                        flux = halo[pair, c, 2 * axis, side(cell, axis)]
                    if spot > 0:
                        back = flow.pop((axis, moved(cell, axis, -1)))
                    else:
                        back = halo[pair, c, 2 * axis + 1, side(cell, axis)]
                    if spot < 2:
                        flow[axis, cell] = flux
                    out = flux - back if out is None else (out + flux) - back
                img[pair, c, cell] = out
                acc = here * out if acc is None else acc + here * out
            if (pair, c) in late:
                partial[pair, c] = acc
            else:
                set_step(pair, c, k, total(acc))

    def finish(k):
        for pair, c in late:
            set_step(pair, c, k, total(partial[pair, c]))

    for n, chain in enumerate(chains):
        far_fluxes(*chain)
        if n >= LEAD:
            near_fluxes(*chains[n - LEAD])
    for chain in chains[len(chains) - LEAD :]:
        near_fluxes(*chain)
    images(0)

    def sweep(k, carry):
        finish(k - 1)
        for pair, c in chains:
            alpha = alphas[pair, c]
            acc = None
            for cell in range(CELLS):
                value = res[pair, c, cell] - alpha * img[pair, c, cell]
                res[pair, c, cell] = value
                acc = value * value if acc is None else acc + value * value
            new = total(acc)
            betas[pair, c] = jnp.where(active(pair, k), new / norms[pair, c], 0.0)
            norms[pair, c] = new
        for n, (pair, c) in enumerate(chains):
            beta = betas[pair, c]
            for cell in range(CELLS):
                value = res[pair, c, cell] + beta * way[pair, c, cell]
                way[pair, c, cell] = value
                path[k, pair, c, cell] = value
            far_fluxes(pair, c)
            if n >= LEAD:
                near_fluxes(*chains[n - LEAD])
        path_copy(k).start()
        for chain in chains[len(chains) - LEAD :]:
            near_fluxes(*chain)
        images(k)
        return carry

    lax.fori_loop(1, most, sweep, 0)
    finish(most - 1)
    steps_copy = pltpu.make_async_copy(steps, steps_hbm, sems.at[9])
    steps_copy.start()

    share = 1.0 / (VOX * YZ)
    packed = zero
    for pair in range(4):
        for d in range(3):
            value = (steps[MICRO_MAX, pair, d] - energy[pair, d]) * share
            packed = jnp.where(lane == d * DEPTH + 2 * pair, value, packed)
            packed = jnp.where(lane == d * DEPTH + 2 * pair + 1, pltpu.roll(value, 64, 1), packed)
    for e in range(DEPTH):
        packed = jnp.where(lane == 3 * DEPTH + e, current_ref[e], packed)
        packed = jnp.where(lane == 4 * DEPTH + e, load_ref[e], packed)
    for block in range(DEVICES // 8):
        packed_ref[block * 8 : block * 8 + 8, :] = packed
    packed_copy = pltpu.make_async_copy(packed_ref, packed_hbm, sems.at[10])
    packed_copy.start()

    def settle(k, carry):
        path_copy(k).wait()
        return carry

    lax.fori_loop(0, most, settle, 0)
    steps_copy.wait()
    packed_copy.wait()


def output_kernel(
    path_hbm,
    steps_hbm,
    back_hbm,
    states_hbm,
    tangent_ref,
    path,
    steps,
    back_ref,
    blocked,
    states_ref,
    sems,
    path_sems,
):
    f32 = jnp.float32
    steps_copy = pltpu.make_async_copy(steps_hbm, steps, sems.at[0])
    steps_copy.start()

    def path_copy(pair, k):
        return pltpu.make_async_copy(path_hbm.at[k, pair], path.at[k, pair], path_sems.at[pair, k])

    for pair in range(2):
        for k in range(MICRO_MIN):
            path_copy(pair, k).start()
    back_copy = pltpu.make_async_copy(back_hbm, back_ref, sems.at[1])
    back_copy.start()
    lane, sub, low, ahead, before, both_halves, total = helpers()
    steps_copy.wait()
    most = jnp.max(steps[MICRO_MAX + 1, 0, 0]).astype(jnp.int32)

    def begin(pair, k, carry):
        path_copy(pair, k).start()
        return carry

    for pair in range(4):
        lax.fori_loop(MICRO_MIN if pair < 2 else 0, most, functools.partial(begin, pair), 0)
    back_copy.wait()

    share = 1.0 / (VOX * YZ)
    row_e = lax.broadcasted_iota(jnp.int32, (16, 128), 1)
    row_d = lax.broadcasted_iota(jnp.int32, (16, 128), 0)
    tangent = jnp.zeros((16, 128), f32)
    rows = 2 * 3 * VOX
    states_copies = []
    for pair in range(4):
        for c in range(3):

            def add(k, held):
                if c == 0:
                    path_copy(pair, k).wait()
                alpha = steps[k, pair, c]
                return tuple(value + alpha * path[k, pair, c, cell] for cell, value in enumerate(held))

            if c == 0:
                for k in range(MICRO_MIN):
                    path_copy(pair, k).wait()
            alpha = [steps[k, pair, c] for k in range(MICRO_MIN)]
            held = []
            for cell in range(CELLS):
                value = alpha[0] * path[0, pair, c, cell]
                for k in range(1, MICRO_MIN):
                    value = value + alpha[k] * path[k, pair, c, cell]
                held.append(value)
            held = lax.fori_loop(MICRO_MIN, most, add, tuple(held))
            accs = [None] * 3
            for cell in range(CELLS):
                for d in range(3):
                    term = held[cell] * path[0, pair, d, cell]
                    accs[d] = term if accs[d] is None else accs[d] + term
            for xi in range(3):
                row = held[xi * 9 : xi * 9 + 9]
                start = c * VOX + xi
                for t in range(5):
                    if t < 4:
                        one = jnp.where(low, row[2 * t], pltpu.roll(row[2 * t + 1], 64, 1))
                        two = jnp.where(low, pltpu.roll(row[2 * t], 64, 1), row[2 * t + 1])
                    else:
                        one = jnp.where(low, row[8], 0.0)
                        two = jnp.where(low, pltpu.roll(row[8], 64, 1), 0.0)
                    blocked[t, pl.ds(start, 8, stride=3), :] = one
                    blocked[t, pl.ds(start + 3 * VOX, 8, stride=3), :] = two
            for d in range(3):
                value = total(accs[d])
                value = (steps[MICRO_MAX, pair, d] - value if d == c else -value) * share
                for half in range(2):
                    flat = value[0:1, 64 * half : 64 * half + 1]
                    tangent = jnp.where((row_d == 3 * d + c) & (row_e == 2 * pair + half), flat, tangent)
        lhs = jnp.concatenate([blocked[t] for t in range(5)], axis=1)
        upper = lhs.astype(jnp.bfloat16)
        lower = (lhs - upper.astype(f32)).astype(jnp.bfloat16)
        both = jnp.dot(jnp.concatenate([upper, lower], axis=0), back_ref[...], preferred_element_type=f32)
        place = pl.ds(pair * rows, rows)
        states_ref[place, :] = both[:rows] + both[rows:]
        states_copies.append(pltpu.make_async_copy(states_ref.at[place], states_hbm.at[place], sems.at[2 + pair]))
        states_copies[pair].start()
    for n in range(9):
        tangent_ref[n] = tangent[n : n + 1, 0:DEPTH]
    for copy in states_copies:
        copy.wait()


def solve_cells(phases, grain, phase_cond, counts, current, load):
    into, back = block_matrices()
    f32 = jnp.float32
    hbm = pl.BlockSpec(memory_space=pltpu.HBM)
    vmem = pl.BlockSpec(memory_space=pltpu.VMEM)
    field = pltpu.VMEM((4, 3, CELLS, 8, 128), f32)
    chain = pltpu.VMEM((4, 3, 8, 128), f32)
    path, steps, packed = pl.pallas_call(
        cells_kernel,
        out_shape=(
            jax.ShapeDtypeStruct((MICRO_MAX, 4, 3, CELLS, 8, 128), f32),
            jax.ShapeDtypeStruct((MICRO_MAX + 2, 4, 3, 8, 128), f32),
            jax.ShapeDtypeStruct((DEVICES, 128), f32),
        ),
        in_specs=[hbm] * 7,
        out_specs=(hbm,) * 3,
        scratch_shapes=[
            pltpu.VMEM((MICRO_MAX, 4, 3, CELLS, 8, 128), f32),
            pltpu.VMEM((MICRO_MAX + 2, 4, 3, 8, 128), f32),
            pltpu.VMEM((DEVICES, 128), f32),
            pltpu.SMEM((3,), f32),
            pltpu.SMEM((DEPTH,), jnp.int32),
            pltpu.SMEM((DEPTH,), f32),
            pltpu.SMEM((DEPTH,), f32),
            pltpu.VMEM((DEPTH * VOX, YZ), jnp.int32),
            pltpu.VMEM((DEPTH * VOX, YZ), f32),
            pltpu.VMEM((YZ, YZ), jnp.bfloat16),
            pltpu.VMEM((5, DEPTH * VOX, 128), f32),
            field,
            field,
            field,
            field,
            pltpu.VMEM((4, 3, 6, 9, 8, 128), f32),
            chain,
            chain,
            chain,
            chain,
            chain,
            pltpu.SemaphoreType.DMA((11,)),
            pltpu.SemaphoreType.DMA((MICRO_MAX,)),
        ],
        compiler_params=pltpu.CompilerParams(vmem_limit_bytes=VMEM),
        name="cells",
    )(phase_cond, counts, current, load, phases, grain, jnp.asarray(into, jnp.bfloat16))

    def output():
        return pl.pallas_call(
            output_kernel,
            out_shape=(
                jax.ShapeDtypeStruct((DEPTH * 3 * VOX, YZ), f32),
                jax.ShapeDtypeStruct((9, 1, DEPTH), f32),
            ),
            in_specs=[hbm] * 3,
            out_specs=(hbm, vmem),
            scratch_shapes=[
                pltpu.VMEM((MICRO_MAX, 4, 3, CELLS, 8, 128), f32),
                pltpu.VMEM((MICRO_MAX + 2, 4, 3, 8, 128), f32),
                pltpu.VMEM((640, YZ), jnp.bfloat16),
                pltpu.VMEM((5, 2 * 3 * VOX, 128), f32),
                pltpu.VMEM((DEPTH * 3 * VOX, YZ), f32),
                pltpu.SemaphoreType.DMA((8,)),
                pltpu.SemaphoreType.DMA((4, MICRO_MAX)),
            ],
            compiler_params=pltpu.CompilerParams(vmem_limit_bytes=VMEM - ROOM),
            cost_estimate=pl.CostEstimate(flops=400_000_000, bytes_accessed=4_000_000, transcendentals=0),
            name="output",
        )(path, steps, jnp.asarray(back, jnp.bfloat16))

    return packed, output


def coarse_kernel(place_ref, packed_ref, increment_ref, residual_ref):
    f32 = jnp.float32
    nodes = packed_ref[...].T
    shape = (DEPTH, DEVICES)
    lane = lax.broadcasted_iota(jnp.int32, shape, 1)
    sub = lax.broadcasted_iota(jnp.int32, shape, 0)
    col, row = lane & (NEY - 1), lane >> 5
    has_next = (row < NEX - 1, col < NEY - 1, sub < DEPTH - 1)
    has_back = (row > 0, col > 0, sub > 0)

    def following(v, axis):
        if axis == 2:
            return pltpu.roll(v, DEPTH - 1, 0)
        return pltpu.roll(v, DEVICES - (NEY if axis == 0 else 1), 1)

    def preceding(v, axis):
        if axis == 2:
            return pltpu.roll(v, 1, 0)
        return pltpu.roll(v, NEY if axis == 0 else 1, 1)

    def total(v):
        v = v[:, :128] + v[:, 128:]
        v = v + pltpu.roll(v, 4, 0)
        v = v + pltpu.roll(v, 2, 0)
        v = v + pltpu.roll(v, 1, 0)
        return jnp.sum(v, axis=1, keepdims=True)

    own = None
    links = []
    for axis in range(3):
        k = nodes[axis * DEPTH : (axis + 1) * DEPTH]
        for shift, inside in ((following, has_next[axis]), (preceding, has_back[axis])):
            other = jnp.where(inside, shift(k, axis), 0.0)
            mean = 0.5 * (k + other)
            own = mean if own is None else own + mean
            links.append((shift, axis, jnp.where(inside, mean, 0.0)))

    def apply(v):
        out = own * v
        for shift, axis, weight in links:
            out = out - weight * shift(v, axis)
        return out

    current = nodes[3 * DEPTH : 4 * DEPTH]
    residual = nodes[4 * DEPTH : 5 * DEPTH] - apply(current)
    increment = direction = trail = norm = step = None
    for iteration in range(MACRO_ITERS):
        image = apply(residual)
        new, curve = total(residual * residual), total(residual * image)
        if iteration == 0:
            step = new / curve
            direction, trail = residual, image
            increment = step * direction
        else:
            ratio = new / norm
            step = new / (curve - ratio * (new / step))
            direction = residual + ratio * direction
            trail = image + ratio * trail
            increment = increment + step * direction
        residual = residual - step * trail
        norm = new

    spot = sub[:, :128] == lane[:, :128]
    for value, ref in ((increment, increment_ref), (residual, residual_ref)):
        column = jnp.sum(jnp.where(lane == place_ref[0], value, 0.0), axis=1, keepdims=True)
        line = jnp.sum(jnp.where(spot, column, 0.0), axis=0, keepdims=True)
        ref[...] = line[:, :DEPTH]


def solve_coarse(place, packed):
    smem = pl.BlockSpec(memory_space=pltpu.SMEM)
    vmem = pl.BlockSpec(memory_space=pltpu.VMEM)
    line = jax.ShapeDtypeStruct((1, DEPTH), jnp.float32)
    return pl.pallas_call(
        coarse_kernel,
        out_shape=(line, line),
        in_specs=[smem, vmem],
        out_specs=(vmem, vmem),
        compiler_params=pltpu.CompilerParams(vmem_limit_bytes=4 * 1024 * 1024),
        name="coarse",
    )(place, packed)


def shards(phases, grain, phase_cond, micro_counts, current, load):
    packed, output = solve_cells(
        phases.reshape(DEPTH * VOX, YZ),
        grain.reshape(DEPTH * VOX, YZ),
        phase_cond,
        micro_counts.reshape(DEPTH),
        current.reshape(DEPTH),
        load.reshape(DEPTH),
    )
    whole = lax.all_to_all(packed.reshape(DEVICES, 1, 128), ROW_COL, 0, 0, tiled=True)
    states, tangent = output()
    place = lax.axis_index(ROW_COL).astype(jnp.int32).reshape(1)
    increment, residual = solve_coarse(place, whole.reshape(DEVICES, 128))
    return (
        states.reshape(1, 1, DEPTH, 3, VOX, YZ),
        tangent.reshape(3, 3, 1, 1, DEPTH).transpose(2, 3, 4, 0, 1),
        increment.reshape(1, 1, DEPTH),
        residual.reshape(1, 1, DEPTH),
    )


def solution(mesh):
    torus = Mesh(mesh.devices.reshape(4, 2, 4, 8), ("row_0", "row_1", "col_0", "col_1"))
    in_specs = (
        P(ROW, COL, None, None, None),
        P(ROW, COL, None, None, None),
        P(),
        P(ROW, COL, None),
        P(ROW, COL, None),
        P(ROW, COL, None),
    )
    out_specs = (
        P(ROW, COL, None, None, None, None),
        P(ROW, COL, None, None, None),
        P(ROW, COL, None),
        P(ROW, COL, None),
    )
    return jax.shard_map(
        shards, mesh=torus, in_specs=in_specs, out_specs=out_specs, check_vma=False
    )
```

```python
import functools

import jax
import jax.numpy as jnp
import numpy as np
from jax import lax
from jax.experimental import pallas as pl
from jax.experimental.pallas import tpu as pltpu
from jax.sharding import Mesh
from jax.sharding import PartitionSpec as P

VOX = 24
YZ = 576
DEPTH = 8
CELLS = 27
MACRO_ITERS = 8
MICRO_MAX = 12
LANE_TAKE = True
MICRO_MIN = 6
VMEM = 67_043_328
ROOM = 400 * 1024
EARLY = 7
LEAD = 12
ROW_COL = ("row_0", "row_1", "col_0", "col_1")
ROW = ("row_0", "row_1")
COL = ("col_0", "col_1")
NEX = 8
NEY = 32
DEVICES = NEX * NEY


def block_order():
    yi, zi, yb, zb = np.meshgrid(np.arange(3), np.arange(3), np.arange(8), np.arange(8), indexing="ij")
    return ((3 * yb + yi) * VOX + 3 * zb + zi).reshape(-1)


def block_matrices():
    order = block_order()
    into = np.zeros((YZ, YZ), np.float32)
    into[order, np.arange(YZ)] = 1.0
    back = np.zeros((640, YZ), np.float32)
    back[np.arange(YZ), order] = 1.0
    return into, back


def at(xi, yi, zi):
    return xi * 9 + yi * 3 + zi


def helpers():
    lane = lax.broadcasted_iota(jnp.int32, (8, 128), 1)
    sub = lax.broadcasted_iota(jnp.int32, (8, 128), 0)
    low = lane < 64
    high_part, yb, zb = lane & 64, (lane >> 3) & 7, lane & 7
    y_part, z_part = lane & 56, lane & 7
    y_next = high_part | ((y_part + 8) & 56) | z_part
    y_prev = high_part | ((y_part + 56) & 56) | z_part
    z_next = high_part | y_part | ((z_part + 1) & 7)
    z_prev = high_part | y_part | ((z_part + 7) & 7)

    def taken(v, index):
        return jnp.take_along_axis(v, index, axis=1, mode="promise_in_bounds")

    if LANE_TAKE:
        ahead = (
            lambda v: pltpu.roll(v, 7, 0),
            lambda v: taken(v, y_next),
            lambda v: taken(v, z_next),
        )
        before = (
            lambda v: pltpu.roll(v, 1, 0),
            lambda v: taken(v, y_prev),
            lambda v: taken(v, z_prev),
        )
    else:
        ahead = (
            lambda v: pltpu.roll(v, 7, 0),
            lambda v: jnp.where(yb == 7, pltpu.roll(v, 56, 1), pltpu.roll(v, 120, 1)),
            lambda v: jnp.where(zb == 7, pltpu.roll(v, 7, 1), pltpu.roll(v, 127, 1)),
        )
        before = (
            lambda v: pltpu.roll(v, 1, 0),
            lambda v: jnp.where(yb == 0, pltpu.roll(v, 72, 1), pltpu.roll(v, 8, 1)),
            lambda v: jnp.where(zb == 0, pltpu.roll(v, 121, 1), pltpu.roll(v, 1, 1)),
        )

    def both_halves(acc):
        acc = acc + pltpu.roll(acc, 4, 0)
        acc = acc + pltpu.roll(acc, 2, 0)
        acc = acc + pltpu.roll(acc, 1, 0)
        first = jnp.sum(jnp.where(low, acc, 0.0), axis=1, keepdims=True)
        second = jnp.sum(jnp.where(low, 0.0, acc), axis=1, keepdims=True)
        return first, second

    def total(acc):
        first, second = both_halves(acc)
        return jnp.where(low, first, second)

    return lane, sub, low, ahead, before, both_halves, total


def coords(cell):
    return cell // 9, (cell // 3) % 3, cell % 3


def side(cell, axis):
    xi, yi, zi = coords(cell)
    return (yi * 3 + zi, xi * 3 + zi, xi * 3 + yi)[axis]


def moved(cell, axis, step):
    spot = list(coords(cell))
    spot[axis] += step
    return at(*spot)


def cells_kernel(
    cond_hbm,
    count_hbm,
    current_hbm,
    load_hbm,
    phase_hbm,
    grain_hbm,
    into_hbm,
    path_hbm,
    steps_hbm,
    packed_hbm,
    path,
    steps,
    packed_ref,
    cond_ref,
    count_ref,
    current_ref,
    load_ref,
    phase_ref,
    grain_ref,
    into_ref,
    native,
    face,
    res,
    way,
    img,
    halo,
    alphas,
    betas,
    norms,
    energy,
    partial,
    sems,
    path_sems,
):
    f32 = jnp.float32
    copies = [
        pltpu.make_async_copy(src, dst, sems.at[n])
        for n, (src, dst) in enumerate(
            (
                (phase_hbm, phase_ref),
                (grain_hbm, grain_ref),
                (into_hbm, into_ref),
                (cond_hbm, cond_ref),
                (count_hbm, count_ref),
                (current_hbm, current_ref),
                (load_hbm, load_ref),
            )
        )
    ]
    for copy in copies:
        copy.start()
    lane, sub, low, ahead, before, both_halves, total = helpers()
    zero = jnp.zeros((8, 128), f32)
    for copy in copies:
        copy.wait()

    phase = phase_ref[...]
    conduct = jnp.where(phase == 0, cond_ref[0], jnp.where(phase == 1, cond_ref[1], cond_ref[2])) * grain_ref[...]
    part_a = conduct.astype(jnp.bfloat16)
    rest = conduct - part_a.astype(f32)
    part_b = rest.astype(jnp.bfloat16)
    into = into_ref[...]
    ordered = jnp.dot(jnp.concatenate([part_a, part_b], axis=0), into, preferred_element_type=f32)
    ordered = ordered[0:192] + ordered[192:384]
    for t in range(4):
        native[t] = ordered[:, t * 128 : (t + 1) * 128]
    native[4, :, 0:64] = ordered[:, 512:576]

    for pair in range(4):
        cells = []
        for xi in range(3):
            for g in range(9):
                first = native[g // 2, pl.ds(2 * pair * VOX + xi, 8, stride=3), :]
                second = native[g // 2, pl.ds((2 * pair + 1) * VOX + xi, 8, stride=3), :]
                if g % 2 == 0:
                    cells.append(jnp.where(low, first, pltpu.roll(second, 64, 1)))
                else:
                    cells.append(jnp.where(low, pltpu.roll(first, 64, 1), second))
        for axis in range(3):
            faces = []
            acc_face = None
            for cell in range(CELLS):
                if coords(cell)[axis] < 2:
                    nxt = cells[moved(cell, axis, 1)]
                else:
                    nxt = ahead[axis](cells[moved(cell, axis, -2)])
                value = (cells[cell] + nxt) * 0.5
                faces.append(value)
                face[pair, axis, cell] = value
                acc_face = value if acc_face is None else acc_face + value
            acc = None
            for cell in range(CELLS):
                if coords(cell)[axis] > 0:
                    back = faces[moved(cell, axis, -1)]
                else:
                    back = before[axis](faces[moved(cell, axis, 2)])
                value = faces[cell] - back
                res[pair, axis, cell] = value
                way[pair, axis, cell] = value
                path[0, pair, axis, cell] = value
                acc = value * value if acc is None else acc + value * value
            norms[pair, axis] = total(acc)
            steps[MICRO_MAX, pair, axis] = total(acc_face)
            energy[pair, axis] = zero

    most = count_ref[0]
    for e in range(1, DEPTH):
        most = jnp.maximum(most, count_ref[e])
    steps[MICRO_MAX + 1, 0, 0] = jnp.full((8, 128), most, jnp.int32).astype(f32)


    def path_copy(k):
        return pltpu.make_async_copy(path.at[k], path_hbm.at[k], path_sems.at[k])

    path_copy(0).start()
    chains = [(pair, c) for pair in range(4) for c in range(3)]
    late = chains[EARLY:]

    def active(pair, k):
        return jnp.where(low, count_ref[2 * pair], count_ref[2 * pair + 1]) > k

    def set_step(pair, c, k, curve):
        norm = norms[pair, c]
        alpha = jnp.where(active(pair, k), norm / curve, 0.0)
        alphas[pair, c] = alpha
        steps[k, pair, c] = alpha
        energy[pair, c] = energy[pair, c] + alpha * norm

    def far_fluxes(pair, c):
        for axis in range(3):
            for cell in range(CELLS):
                if coords(cell)[axis] == 2:
                    nxt = ahead[axis](way[pair, c, moved(cell, axis, -2)])
                    halo[pair, c, 2 * axis, side(cell, axis)] = face[pair, axis, cell] * (way[pair, c, cell] - nxt)

    def near_fluxes(pair, c):
        for axis in range(3):
            for spot in range(9):
                halo[pair, c, 2 * axis + 1, spot] = before[axis](halo[pair, c, 2 * axis, spot])

    def images(k):
        for pair, c in chains:
            flow = {}
            acc = None
            for cell in range(CELLS):
                here = way[pair, c, cell]
                out = None
                for axis in range(3):
                    spot = coords(cell)[axis]
                    if spot < 2:
                        flux = face[pair, axis, cell] * (here - way[pair, c, moved(cell, axis, 1)])
                    else:
                        flux = halo[pair, c, 2 * axis, side(cell, axis)]
                    if spot > 0:
                        back = flow.pop((axis, moved(cell, axis, -1)))
                    else:
                        back = halo[pair, c, 2 * axis + 1, side(cell, axis)]
                    if spot < 2:
                        flow[axis, cell] = flux
                    out = flux - back if out is None else (out + flux) - back
                img[pair, c, cell] = out
                acc = here * out if acc is None else acc + here * out
            if (pair, c) in late:
                partial[pair, c] = acc
            else:
                set_step(pair, c, k, total(acc))

    def finish(k):
        for pair, c in late:
            set_step(pair, c, k, total(partial[pair, c]))

    for n, chain in enumerate(chains):
        far_fluxes(*chain)
        if n >= LEAD:
            near_fluxes(*chains[n - LEAD])
    for chain in chains[len(chains) - LEAD :]:
        near_fluxes(*chain)
    images(0)

    def sweep(k, carry):
        finish(k - 1)
        for pair, c in chains:
            alpha = alphas[pair, c]
            acc = None
            for cell in range(CELLS):
                value = res[pair, c, cell] - alpha * img[pair, c, cell]
                res[pair, c, cell] = value
                acc = value * value if acc is None else acc + value * value
            new = total(acc)
            betas[pair, c] = jnp.where(active(pair, k), new / norms[pair, c], 0.0)
            norms[pair, c] = new
        for n, (pair, c) in enumerate(chains):
            beta = betas[pair, c]
            for cell in range(CELLS):
                value = res[pair, c, cell] + beta * way[pair, c, cell]
                way[pair, c, cell] = value
                path[k, pair, c, cell] = value
            far_fluxes(pair, c)
            if n >= LEAD:
                near_fluxes(*chains[n - LEAD])
        path_copy(k).start()
        for chain in chains[len(chains) - LEAD :]:
            near_fluxes(*chain)
        images(k)
        return carry

    lax.fori_loop(1, most, sweep, 0)
    finish(most - 1)
    steps_copy = pltpu.make_async_copy(steps, steps_hbm, sems.at[9])
    steps_copy.start()

    share = 1.0 / (VOX * YZ)
    packed = zero
    for pair in range(4):
        for d in range(3):
            value = (steps[MICRO_MAX, pair, d] - energy[pair, d]) * share
            packed = jnp.where(lane == d * DEPTH + 2 * pair, value, packed)
            packed = jnp.where(lane == d * DEPTH + 2 * pair + 1, pltpu.roll(value, 64, 1), packed)
    for e in range(DEPTH):
        packed = jnp.where(lane == 3 * DEPTH + e, current_ref[e], packed)
        packed = jnp.where(lane == 4 * DEPTH + e, load_ref[e], packed)
    for block in range(DEVICES // 8):
        packed_ref[block * 8 : block * 8 + 8, :] = packed
    packed_copy = pltpu.make_async_copy(packed_ref, packed_hbm, sems.at[10])
    packed_copy.start()

    def settle(k, carry):
        path_copy(k).wait()
        return carry

    lax.fori_loop(0, most, settle, 0)
    steps_copy.wait()
    packed_copy.wait()


def output_kernel(
    path_hbm,
    steps_hbm,
    back_hbm,
    states_hbm,
    tangent_ref,
    path,
    steps,
    back_ref,
    blocked,
    states_ref,
    sems,
    path_sems,
):
    f32 = jnp.float32
    steps_copy = pltpu.make_async_copy(steps_hbm, steps, sems.at[0])
    steps_copy.start()

    def path_copy(pair, k):
        return pltpu.make_async_copy(path_hbm.at[k, pair], path.at[k, pair], path_sems.at[pair, k])

    for pair in range(2):
        for k in range(MICRO_MIN):
            path_copy(pair, k).start()
    back_copy = pltpu.make_async_copy(back_hbm, back_ref, sems.at[1])
    back_copy.start()
    lane, sub, low, ahead, before, both_halves, total = helpers()
    steps_copy.wait()
    most = jnp.max(steps[MICRO_MAX + 1, 0, 0]).astype(jnp.int32)

    def begin(pair, k, carry):
        path_copy(pair, k).start()
        return carry

    for pair in range(4):
        lax.fori_loop(MICRO_MIN if pair < 2 else 0, most, functools.partial(begin, pair), 0)
    back_copy.wait()

    share = 1.0 / (VOX * YZ)
    row_e = lax.broadcasted_iota(jnp.int32, (16, 128), 1)
    row_d = lax.broadcasted_iota(jnp.int32, (16, 128), 0)
    tangent = jnp.zeros((16, 128), f32)
    rows = 2 * 3 * VOX
    states_copies = []
    for pair in range(4):
        for c in range(3):

            def add(k, held):
                if c == 0:
                    path_copy(pair, k).wait()
                alpha = steps[k, pair, c]
                return tuple(value + alpha * path[k, pair, c, cell] for cell, value in enumerate(held))

            if c == 0:
                for k in range(MICRO_MIN):
                    path_copy(pair, k).wait()
            alpha = [steps[k, pair, c] for k in range(MICRO_MIN)]
            held = []
            for cell in range(CELLS):
                value = alpha[0] * path[0, pair, c, cell]
                for k in range(1, MICRO_MIN):
                    value = value + alpha[k] * path[k, pair, c, cell]
                held.append(value)
            held = lax.fori_loop(MICRO_MIN, most, add, tuple(held))
            accs = [None] * 3
            for cell in range(CELLS):
                for d in range(3):
                    term = held[cell] * path[0, pair, d, cell]
                    accs[d] = term if accs[d] is None else accs[d] + term
            for xi in range(3):
                row = held[xi * 9 : xi * 9 + 9]
                start = c * VOX + xi
                for t in range(5):
                    if t < 4:
                        one = jnp.where(low, row[2 * t], pltpu.roll(row[2 * t + 1], 64, 1))
                        two = jnp.where(low, pltpu.roll(row[2 * t], 64, 1), row[2 * t + 1])
                    else:
                        one = jnp.where(low, row[8], 0.0)
                        two = jnp.where(low, pltpu.roll(row[8], 64, 1), 0.0)
                    blocked[t, pl.ds(start, 8, stride=3), :] = one
                    blocked[t, pl.ds(start + 3 * VOX, 8, stride=3), :] = two
            for d in range(3):
                value = total(accs[d])
                value = (steps[MICRO_MAX, pair, d] - value if d == c else -value) * share
                for half in range(2):
                    flat = value[0:1, 64 * half : 64 * half + 1]
                    tangent = jnp.where((row_d == 3 * d + c) & (row_e == 2 * pair + half), flat, tangent)
        lhs = jnp.concatenate([blocked[t] for t in range(5)], axis=1)
        upper = lhs.astype(jnp.bfloat16)
        lower = (lhs - upper.astype(f32)).astype(jnp.bfloat16)
        both = jnp.dot(jnp.concatenate([upper, lower], axis=0), back_ref[...], preferred_element_type=f32)
        place = pl.ds(pair * rows, rows)
        states_ref[place, :] = both[:rows] + both[rows:]
        states_copies.append(pltpu.make_async_copy(states_ref.at[place], states_hbm.at[place], sems.at[2 + pair]))
        states_copies[pair].start()
    for n in range(9):
        tangent_ref[n] = tangent[n : n + 1, 0:DEPTH]
    for copy in states_copies:
        copy.wait()


def solve_cells(phases, grain, phase_cond, counts, current, load):
    into, back = block_matrices()
    f32 = jnp.float32
    hbm = pl.BlockSpec(memory_space=pltpu.HBM)
    vmem = pl.BlockSpec(memory_space=pltpu.VMEM)
    field = pltpu.VMEM((4, 3, CELLS, 8, 128), f32)
    chain = pltpu.VMEM((4, 3, 8, 128), f32)
    path, steps, packed = pl.pallas_call(
        cells_kernel,
        out_shape=(
            jax.ShapeDtypeStruct((MICRO_MAX, 4, 3, CELLS, 8, 128), f32),
            jax.ShapeDtypeStruct((MICRO_MAX + 2, 4, 3, 8, 128), f32),
            jax.ShapeDtypeStruct((DEVICES, 128), f32),
        ),
        in_specs=[hbm] * 7,
        out_specs=(hbm,) * 3,
        scratch_shapes=[
            pltpu.VMEM((MICRO_MAX, 4, 3, CELLS, 8, 128), f32),
            pltpu.VMEM((MICRO_MAX + 2, 4, 3, 8, 128), f32),
            pltpu.VMEM((DEVICES, 128), f32),
            pltpu.SMEM((3,), f32),
            pltpu.SMEM((DEPTH,), jnp.int32),
            pltpu.SMEM((DEPTH,), f32),
            pltpu.SMEM((DEPTH,), f32),
            pltpu.VMEM((DEPTH * VOX, YZ), jnp.int32),
            pltpu.VMEM((DEPTH * VOX, YZ), f32),
            pltpu.VMEM((YZ, YZ), jnp.bfloat16),
            pltpu.VMEM((5, DEPTH * VOX, 128), f32),
            field,
            field,
            field,
            field,
            pltpu.VMEM((4, 3, 6, 9, 8, 128), f32),
            chain,
            chain,
            chain,
            chain,
            chain,
            pltpu.SemaphoreType.DMA((11,)),
            pltpu.SemaphoreType.DMA((MICRO_MAX,)),
        ],
        compiler_params=pltpu.CompilerParams(vmem_limit_bytes=VMEM),
        name="cells",
    )(phase_cond, counts, current, load, phases, grain, jnp.asarray(into, jnp.bfloat16))

    def output():
        return pl.pallas_call(
            output_kernel,
            out_shape=(
                jax.ShapeDtypeStruct((DEPTH * 3 * VOX, YZ), f32),
                jax.ShapeDtypeStruct((9, 1, DEPTH), f32),
            ),
            in_specs=[hbm] * 3,
            out_specs=(hbm, vmem),
            scratch_shapes=[
                pltpu.VMEM((MICRO_MAX, 4, 3, CELLS, 8, 128), f32),
                pltpu.VMEM((MICRO_MAX + 2, 4, 3, 8, 128), f32),
                pltpu.VMEM((640, YZ), jnp.bfloat16),
                pltpu.VMEM((5, 2 * 3 * VOX, 128), f32),
                pltpu.VMEM((DEPTH * 3 * VOX, YZ), f32),
                pltpu.SemaphoreType.DMA((8,)),
                pltpu.SemaphoreType.DMA((4, MICRO_MAX)),
            ],
            compiler_params=pltpu.CompilerParams(vmem_limit_bytes=VMEM - ROOM),
            cost_estimate=pl.CostEstimate(flops=400_000_000, bytes_accessed=4_000_000, transcendentals=0),
            name="output",
        )(path, steps, jnp.asarray(back, jnp.bfloat16))

    return packed, output


def coarse_kernel(place_ref, packed_ref, increment_ref, residual_ref):
    f32 = jnp.float32
    nodes = packed_ref[...].T
    shape = (DEPTH, DEVICES)
    lane = lax.broadcasted_iota(jnp.int32, shape, 1)
    sub = lax.broadcasted_iota(jnp.int32, shape, 0)
    col, row = lane & (NEY - 1), lane >> 5
    has_next = (row < NEX - 1, col < NEY - 1, sub < DEPTH - 1)
    has_back = (row > 0, col > 0, sub > 0)

    def following(v, axis):
        if axis == 2:
            return pltpu.roll(v, DEPTH - 1, 0)
        return pltpu.roll(v, DEVICES - (NEY if axis == 0 else 1), 1)

    def preceding(v, axis):
        if axis == 2:
            return pltpu.roll(v, 1, 0)
        return pltpu.roll(v, NEY if axis == 0 else 1, 1)

    def total(v):
        v = v[:, :128] + v[:, 128:]
        v = v + pltpu.roll(v, 4, 0)
        v = v + pltpu.roll(v, 2, 0)
        v = v + pltpu.roll(v, 1, 0)
        return jnp.sum(v, axis=1, keepdims=True)

    own = None
    links = []
    for axis in range(3):
        k = nodes[axis * DEPTH : (axis + 1) * DEPTH]
        for shift, inside in ((following, has_next[axis]), (preceding, has_back[axis])):
            other = jnp.where(inside, shift(k, axis), 0.0)
            mean = 0.5 * (k + other)
            own = mean if own is None else own + mean
            links.append((shift, axis, jnp.where(inside, mean, 0.0)))

    def apply(v):
        out = own * v
        for shift, axis, weight in links:
            out = out - weight * shift(v, axis)
        return out

    current = nodes[3 * DEPTH : 4 * DEPTH]
    residual = nodes[4 * DEPTH : 5 * DEPTH] - apply(current)
    increment = direction = trail = norm = step = None
    for iteration in range(MACRO_ITERS):
        image = apply(residual)
        new, curve = total(residual * residual), total(residual * image)
        if iteration == 0:
            step = new / curve
            direction, trail = residual, image
            increment = step * direction
        else:
            ratio = new / norm
            step = new / (curve - ratio * (new / step))
            direction = residual + ratio * direction
            trail = image + ratio * trail
            increment = increment + step * direction
        residual = residual - step * trail
        norm = new

    spot = sub[:, :128] == lane[:, :128]
    for value, ref in ((increment, increment_ref), (residual, residual_ref)):
        column = jnp.sum(jnp.where(lane == place_ref[0], value, 0.0), axis=1, keepdims=True)
        line = jnp.sum(jnp.where(spot, column, 0.0), axis=0, keepdims=True)
        ref[...] = line[:, :DEPTH]


def solve_coarse(place, packed):
    smem = pl.BlockSpec(memory_space=pltpu.SMEM)
    vmem = pl.BlockSpec(memory_space=pltpu.VMEM)
    line = jax.ShapeDtypeStruct((1, DEPTH), jnp.float32)
    return pl.pallas_call(
        coarse_kernel,
        out_shape=(line, line),
        in_specs=[smem, vmem],
        out_specs=(vmem, vmem),
        compiler_params=pltpu.CompilerParams(vmem_limit_bytes=4 * 1024 * 1024),
        name="coarse",
    )(place, packed)


def shards(phases, grain, phase_cond, micro_counts, current, load):
    packed, output = solve_cells(
        phases.reshape(DEPTH * VOX, YZ),
        grain.reshape(DEPTH * VOX, YZ),
        phase_cond,
        micro_counts.reshape(DEPTH),
        current.reshape(DEPTH),
        load.reshape(DEPTH),
    )
    whole = lax.all_to_all(packed.reshape(DEVICES, 1, 128), ROW_COL, 0, 0, tiled=True)
    states, tangent = output()
    place = lax.axis_index(ROW_COL).astype(jnp.int32).reshape(1)
    increment, residual = solve_coarse(place, whole.reshape(DEVICES, 128))
    return (
        states.reshape(1, 1, DEPTH, 3, VOX, YZ),
        tangent.reshape(3, 3, 1, 1, DEPTH).transpose(2, 3, 4, 0, 1),
        increment.reshape(1, 1, DEPTH),
        residual.reshape(1, 1, DEPTH),
    )


def solution(mesh):
    torus = Mesh(mesh.devices.reshape(4, 2, 4, 8), ("row_0", "row_1", "col_0", "col_1"))
    in_specs = (
        P(ROW, COL, None, None, None),
        P(ROW, COL, None, None, None),
        P(),
        P(ROW, COL, None),
        P(ROW, COL, None),
        P(ROW, COL, None),
    )
    out_specs = (
        P(ROW, COL, None, None, None, None),
        P(ROW, COL, None, None, None),
        P(ROW, COL, None),
        P(ROW, COL, None),
    )
    return jax.shard_map(
        shards, mesh=torus, in_specs=in_specs, out_specs=out_specs, check_vma=False
    )
```
